32 devices in a mesh: dom: 8 (over y, x, core), col: 4 (over z).
Axes of the slice: x: 2, y: 2, z: 4, core: 2. Of those that a mesh axis runs over, the one named last changes fastest.
Arguments:
- features: bfloat16 [65536, 1024], P('dom', 'col')
- weight: bfloat16 [1024, 1024], P(None, 'col'), may hold values from -0.1875 to 0.1875
- out_bias: bfloat16 [1024], P('col'), may hold values from -3 to 3
- local_index: int32 [8, 64, 4], P('dom'), may hold values from 0 to 63
- local_count: int32 [8, 64], P('dom'), may hold values from 1 to 4, as said below
- local_vals: bfloat16 [8, 64, 4, 128, 128], P('dom'), may hold values from -0.1875 to 0.1875
- halo_index: int32 [8, 64, 4], P('dom'), may hold values from 0 to 31
- halo_count: int32 [8, 64], P('dom'), may hold values from 0 to 4, as said below
- halo_vals: bfloat16 [8, 64, 4, 128, 128], P('dom'), may hold values from -0.1875 to 0.1875
- send_rows: int32 [8, 8, 512], P('dom'), may hold values from 0 to 8191
- send_count: int32 [8, 8], P('dom'), may hold values from 0 to 512, as said below
Outputs:
- normalized: bfloat16 [65536, 1024], P('dom', 'col')
- channel_stats: float32 [2, 1024], P(None, 'col')
The draws below stay inside these ranges and needn't reach their ends.
Inputs may be any that keep to these rules, and one draw needn't show every extreme that they name: `local_index`: slots k >= local_count of a row tile are not used. `local_count`: every partition has a row tile with all 4 slots used. `halo_index`: slots k >= halo_count of a row tile are not used. `halo_count`: every partition has a row tile with all 4 slots used. `send_rows`: slots s >= send_count[q, p] are not used. send_count[p, p] is 0; every partition fills all 512 slots to some other partition.
All inputs are finite; a program needn't handle non-finite values.
Results may differ from the reference program's by a relative error of at most 0.0075.
Values may be sent and summed in bfloat16 or wider, within the bound.
A program may use at most 192 MiB of HBM per device.

```python
import jax
import jax.numpy as jnp
from jax import lax

F = 1024
ROWS_DEV = 8192
TILE = 128
LOCAL_SLOTS = 4
HALO_SLOTS = 4
HALO_PEER = 512
NODES = 65536
LOCAL_TILES = 64
HALO_TILES = 32
N_DOM = 8


def draw_features(key, part):
    key_base = jax.random.fold_in(key, 0)
    rising = 1.0 + 2.0 * jnp.arange(NODES, dtype=jnp.float32) / NODES
    values = jax.random.normal(key_base, (NODES, F), jnp.float32) * rising[:, None]
    return values.astype(jnp.bfloat16)


def slot_counts(key, highest, lowest):
    key_base, key_heavy, key_place = jax.random.split(key, 3)
    counts = jax.random.randint(key_base, (N_DOM, LOCAL_TILES), lowest, highest + 1)
    heavier = jax.random.randint(key_heavy, (N_DOM, 1), 0, highest)
    counts = jnp.minimum(counts + heavier, highest)
    placed = jax.random.randint(key_place, (N_DOM, 1), 0, LOCAL_TILES)
    tile_ids = jnp.arange(LOCAL_TILES)[None, :]
    return jnp.where(tile_ids == placed, highest, counts).astype(jnp.int32)


def draw_local_count(key, part):
    return slot_counts(jax.random.fold_in(key, 11), LOCAL_SLOTS, 1)


def draw_halo_count(key, part):
    return slot_counts(jax.random.fold_in(key, 23), HALO_SLOTS, 0)


def draw_send_count(key, part):
    key_base, key_target = jax.random.split(jax.random.fold_in(key, 37))
    counts = jax.random.randint(key_base, (N_DOM, N_DOM), HALO_PEER // 4, HALO_PEER + 1)
    offset = jax.random.randint(key_target, (N_DOM, 1), 1, N_DOM)
    sources = jnp.arange(N_DOM)[:, None]
    targets = jnp.arange(N_DOM)[None, :]
    counts = jnp.where(targets == (sources + offset) % N_DOM, HALO_PEER, counts)
    return jnp.where(targets == sources, 0, counts).astype(jnp.int32)


def touch_ends(entries, key, low, high):
    longest = entries.shape.index(max(entries.shape))
    spots = []
    for shift in (0, 1):
        where = [jax.random.randint(jax.random.fold_in(key, axis), (), 0, length) for axis, length in enumerate(entries.shape)]
        where[longest] = (where[longest] + shift) % entries.shape[longest]
        spots.append(tuple(where))
    return entries.at[spots[0]].set(low).at[spots[1]].set(high)


def block_levels(stream_key, shape, cuts, least, high):
    level = 1.0
    for dim, shards_of in cuts:
        draws = jax.random.uniform(jax.random.fold_in(jax.random.fold_in(stream_key, 6), dim), (shards_of,), jnp.float32, least / len(cuts), high / len(cuts))
        level = level * jnp.repeat(jnp.exp(draws), shape[dim] // shards_of).reshape((-1,) + (1,) * (len(shape) - 1 - dim))
    return level


def bell_draw(stream_key, dims, deviation, reach, cuts=(), kind=jnp.bfloat16):
    entries = deviation * jax.random.normal(stream_key, dims, jnp.float32)
    if cuts:
        entries = entries * block_levels(stream_key, dims, cuts, -0.22, 0.18)
    return jnp.clip(entries, -reach, reach).astype(kind)


def setup_inputs(seed: int = 0) -> dict:
    arg_keys = jax.random.split(jax.random.key(seed), 12)
    features = draw_features(jax.random.fold_in(arg_keys[11], 71), 0)
    weight = bell_draw(arg_keys[1], (F, F), F ** -0.5, 0.1875, ((1, 4),))
    out_bias = bell_draw(arg_keys[2], (F,), 0.5, 3.0, ((0, 4),))
    local_index = touch_ends(jax.random.randint(arg_keys[3], (N_DOM, LOCAL_TILES, LOCAL_SLOTS), 0, LOCAL_TILES), jax.random.fold_in(arg_keys[3], 1), 0, LOCAL_TILES - 1).astype(jnp.int32)
    local_count = draw_local_count(jax.random.fold_in(arg_keys[11], 71), 0)
    local_vals = bell_draw(arg_keys[5], (N_DOM, LOCAL_TILES, LOCAL_SLOTS, TILE, TILE), (TILE * (LOCAL_SLOTS + HALO_SLOTS)) ** -0.5, 0.1875, ((0, 8),))
    halo_index = touch_ends(jax.random.randint(arg_keys[6], (N_DOM, LOCAL_TILES, HALO_SLOTS), 0, HALO_TILES), jax.random.fold_in(arg_keys[6], 1), 0, HALO_TILES - 1).astype(jnp.int32)
    halo_count = draw_halo_count(jax.random.fold_in(arg_keys[11], 71), 0)
    halo_vals = bell_draw(arg_keys[8], (N_DOM, LOCAL_TILES, HALO_SLOTS, TILE, TILE), (TILE * (LOCAL_SLOTS + HALO_SLOTS)) ** -0.5, 0.1875, ((0, 8),))
    send_rows = touch_ends(jax.random.randint(arg_keys[9], (N_DOM, N_DOM, HALO_PEER), 0, ROWS_DEV), jax.random.fold_in(arg_keys[9], 1), 0, ROWS_DEV - 1).astype(jnp.int32)
    send_count = draw_send_count(jax.random.fold_in(arg_keys[11], 71), 0)
    return {"features": features, "weight": weight, "out_bias": out_bias, "local_index": local_index, "local_count": local_count, "local_vals": local_vals, "halo_index": halo_index, "halo_count": halo_count, "halo_vals": halo_vals, "send_rows": send_rows, "send_count": send_count}


epsilon = 1e-06

def tile_product(sources, tile_index, tile_count, tile_vals, slot_total):
    gathered = sources[tile_index]
    keep_mask = jnp.arange(slot_total)[None, :] < tile_count[:, None]
    masked = jnp.where(keep_mask[:, :, None, None], tile_vals, jnp.zeros_like(tile_vals))
    return jnp.einsum('tkij,tkjc->tic', masked.astype(jnp.float32), gathered.astype(jnp.float32))

def reference(features, weight, out_bias, local_index, local_count, local_vals, halo_index, halo_count, halo_vals, send_rows, send_count):
    blocks = features.reshape(N_DOM, ROWS_DEV, F)
    slot_ids = jnp.arange(HALO_PEER)
    sources_ids = jnp.arange(N_DOM)

    def aggregate(partition):
        chosen = blocks[sources_ids[:, None], send_rows[:, partition, :]]
        keep_mask = slot_ids[None, :] < send_count[:, partition][:, None]
        halo_tiles = jnp.where(keep_mask[:, :, None], chosen, jnp.zeros_like(chosen)).reshape(HALO_TILES, TILE, F)
        own_tiles = blocks[partition].reshape(LOCAL_TILES, TILE, F)
        summed = tile_product(own_tiles, local_index[partition], local_count[partition], local_vals[partition], LOCAL_SLOTS)
        summed = summed + tile_product(halo_tiles, halo_index[partition], halo_count[partition], halo_vals[partition], HALO_SLOTS)
        return summed.reshape(ROWS_DEV, F).astype(jnp.bfloat16)
    spread = lax.map(aggregate, jnp.arange(N_DOM)).reshape(NODES, F)
    mixed_rows = jnp.dot(spread, weight, preferred_element_type=jnp.float32) + out_bias.astype(jnp.float32)
    active = jnp.maximum(mixed_rows, 0.0)
    row_power = lax.optimization_barrier(jnp.mean(active * active, axis=1, keepdims=True))
    scaled = active * lax.rsqrt(row_power + epsilon)
    channel_mean = lax.optimization_barrier(jnp.sum(scaled, axis=0)) / NODES
    channel_var = lax.optimization_barrier(jnp.sum(scaled * scaled, axis=0)) / NODES - channel_mean * channel_mean
    return (scaled.astype(jnp.bfloat16), jnp.stack([channel_mean, channel_var]))
```

```python
import functools

import jax
import jax.numpy as jnp
from jax import lax
from jax.experimental import pallas as pl
from jax.experimental.pallas import tpu as pltpu
from jax.sharding import PartitionSpec as P

TILE = 128
MESH = pl.DeviceIdType.MESH
LANES = 128
P1_TILES = 4
P2_TILES = 2
epsilon = 1e-06


def remote(src, dst, send_sem, recv_sem, device):
    return pltpu.make_async_remote_copy(
        src_ref=src,
        dst_ref=dst,
        send_sem=send_sem,
        recv_sem=recv_sem,
        device_id=device,
        device_id_type=MESH,
    )


def kernel(
    n_dom,
    n_col,
    node_total,
    feat_hbm,
    weight_hbm,
    bias_ref,
    lidx,
    lcnt,
    lvals_hbm,
    hidx,
    hcnt,
    hvals_hbm,
    srows,
    scnt,
    out_hbm,
    stat_ref,
    xb,
    xf,
    stage,
    outgoing,
    halo_a,
    halo_b,
    lvals,
    hvals,
    wfull,
    bfull,
    tx,
    rx,
    tx2,
    acc,
    part,
    part_in,
    colpart,
    colpart_in,
    feat_sem,
    vals_sem,
    wl_sem,
    halo_s,
    halo_r,
    w_s,
    w_r,
    wp_s,
    wp_r,
    b_s,
    b_r,
    p1_s,
    p1_r,
    p2_s,
    p2_r,
    own_sem,
    sd_s,
    sd_r,
    sc_s,
    sc_r,
):
    d = lax.axis_index("dom")
    z = lax.axis_index("col")
    halos = (halo_a, halo_b)
    n_part, rows, lanes = xf.shape
    width = n_part * lanes
    slot_total = srows.shape[1]
    k_local = lvals.shape[1]
    k_halo = hvals.shape[1]
    f_total = weight_hbm.shape[0]
    tiles_q = rows // TILE // n_col
    rows_q = tiles_q * TILE
    ct = P1_TILES
    r_chunk = ct * TILE
    steps = tiles_q // ct
    r_out = P2_TILES * TILE
    halves = r_chunk // r_out
    per_peer = slot_total // TILE
    shard = f_total // n_dom
    n_chips = n_dom // 2
    chip = d // 2
    core = lax.rem(d, 2)
    mate = d + 1 - 2 * core

    pieces = feat_sem.shape[1]
    piece = rows // TILE // pieces

    def feat_copy(c, i):
        at = pl.ds(i * piece, piece)
        return pltpu.make_async_copy(
            feat_hbm.at[at, :, pl.ds(c * lanes, lanes)], xb.at[c, at], feat_sem.at[c, i]
        )

    def w_load():
        mine = pl.ds(pl.multiple_of(d * shard, shard), shard)
        return pltpu.make_async_copy(weight_hbm.at[mine], wfull.at[z, d], wl_sem)

    for i in range(pieces):
        feat_copy(0, i).start()
    w_load().start()
    for i in range(pieces):
        feat_copy(1, i).start()
    bfull[z] = jnp.broadcast_to(bias_ref[...], bfull.shape[1:])

    barrier = pltpu.get_barrier_semaphore()
    for o in range(1, n_dom):
        pl.semaphore_signal(barrier, inc=1, device_id=(lax.rem(d + o, n_dom), z), device_id_type=MESH)
    for o in range(1, n_col):
        pl.semaphore_signal(barrier, inc=1, device_id=(d, lax.rem(z + o, n_col)), device_id_type=MESH)
    pl.semaphore_wait(barrier, n_dom - 1 + n_col - 1)

    def w_copy(o):
        return remote(
            wfull.at[z, d], wfull.at[z, d], w_s.at[o - 1], w_r.at[o - 1], (d, lax.rem(z + o, n_col))
        )

    def w_arrived(o):
        src = lax.rem(z + n_col - o, n_col)
        return remote(
            wfull.at[src, d], wfull.at[src, d], w_s.at[o - 1], w_r.at[o - 1], (d, src)
        )

    def w_pass(o):
        return remote(
            wfull.at[:, d], wfull.at[:, d], wp_s.at[o], wp_r.at[o], (lax.rem(d + o, n_dom), z)
        )

    def w_passed(o):
        src = lax.rem(d + n_dom - o, n_dom)
        return remote(wfull.at[:, src], wfull.at[:, src], wp_s.at[o], wp_r.at[o], (src, z))

    def b_copy(o):
        return remote(
            bfull.at[z], bfull.at[z], b_s.at[o - 1], b_r.at[o - 1], (d, lax.rem(z + o, n_col))
        )

    w_load().wait()
    for o in range(1, n_col):
        w_copy(o).start()
        b_copy(o).start()

    def widen(c):
        @pl.loop(0, pieces)
        def _(i):
            feat_copy(c, i).wait()
            for j in range(piece):
                t = i * piece + j
                xf[c, pl.ds(pl.multiple_of(t * TILE, TILE), TILE), :] = xb[c, t].astype(jnp.float32)

    def slots_of(q):
        return pl.ds(q * per_peer, per_peer)

    def halo_send(c, peer):
        return remote(
            outgoing.at[c, peer],
            halos[c].at[slots_of(d)],
            halo_s.at[c, peer],
            halo_r.at[c, d],
            (peer, z),
        )

    def halo_arrived(c, src):
        return remote(
            outgoing.at[c, src],
            halos[c].at[slots_of(src)],
            halo_s.at[c, src],
            halo_r.at[c, src],
            (src, z),
        )

    def gather(c, peer):
        @pl.loop(0, slot_total // 16)
        def _(g):
            for k in range(16):
                at = g * 16 + k
                stage[at] = xf[c, srows[peer, at]]

        used = lax.broadcasted_iota(jnp.int32, (slot_total, lanes), 0) < scnt[0, peer]
        sent = jnp.where(used, stage[...], 0.0).astype(outgoing.dtype)
        outgoing[c, peer] = sent.reshape(per_peer, TILE, lanes)
        halo_send(c, peer).start()

    def gather_all(c):
        @pl.loop(1, n_chips)
        def _(j):
            gather(c, 2 * lax.rem(chip + j, n_chips))

        gather(c, mate)

        @pl.loop(1, n_chips)
        def _(j):
            gather(c, 2 * lax.rem(chip + j, n_chips) + 1)

    lv_copy = pltpu.make_async_copy(lvals_hbm, lvals, vals_sem.at[0])
    hv_copy = pltpu.make_async_copy(hvals_hbm, hvals, vals_sem.at[1])

    widen(0)
    lv_copy.start()
    hv_copy.start()
    gather_all(0)
    widen(1)
    gather_all(1)
    for c in range(n_part):
        halos[c][slots_of(d)] = jnp.zeros((per_peer, TILE, lanes), halo_a.dtype)

    lv_copy.wait()
    hv_copy.wait()

    def kept(count, k):
        one = jnp.minimum(jnp.maximum(count - k, 0), 1).astype(jnp.float32)
        return jnp.broadcast_to(one, (TILE, TILE)).astype(jnp.bfloat16)

    def tile_rows(c, t):
        lhs, rhs = [], []
        n_loc, n_hal = lcnt[0, t], hcnt[0, t]
        for k in range(k_local):
            lhs.append(lvals[t, k] * kept(n_loc, k))
            rhs.append(xb[c, lidx[k, t]])
        for k in range(k_halo):
            lhs.append(hvals[t, k] * kept(n_hal, k))
            rhs.append(halos[c][hidx[k, t]])
        total = jnp.dot(
            jnp.concatenate(lhs, axis=1),
            jnp.concatenate(rhs, axis=0),
            preferred_element_type=jnp.float32,
        )
        return total.astype(jnp.bfloat16)

    def my_cols(c):
        return pl.ds(pl.multiple_of(z * width + c * lanes, lanes), lanes)

    def p1_copy(c, s, o):
        return remote(
            tx.at[c, s, o - 1],
            rx.at[s, :, my_cols(c)],
            p1_s.at[c, s, o - 1],
            p1_r.at[c, s, o - 1],
            (d, lax.rem(z + o, n_col)),
        )

    for c in range(n_part):

        @pl.loop(1, n_dom)
        def _(o):
            halo_arrived(c, lax.rem(d + o, n_dom)).wait_recv()

        @pl.loop(0, steps)
        def _(s):
            for o in range(1, n_col):
                q = lax.rem(z + o, n_col)
                for i in range(ct):
                    tx[c, s, o - 1, i * TILE : (i + 1) * TILE, :] = tile_rows(c, q * tiles_q + s * ct + i)
                p1_copy(c, s, o).start()
            for i in range(ct):
                rx[s, i * TILE : (i + 1) * TILE, my_cols(c)] = tile_rows(c, z * tiles_q + s * ct + i)

        if c == 0:
            for o in range(1, n_col):
                w_arrived(o).wait_recv()

            @pl.loop(1, n_dom)
            def _(o):
                w_pass(o).start()

    @pl.loop(1, n_dom)
    def _(o):
        w_passed(o).wait_recv()

    for o in range(1, n_col):
        b_copy(o).wait()

    acc[...] = jnp.zeros_like(acc)

    def out_rows(s):
        return pl.ds(pl.multiple_of(z * rows_q + s * r_out, r_out), r_out)

    def p2_copy(s, o):
        q = lax.rem(z + o, n_col)
        return remote(
            tx2.at[s, q],
            out_hbm.at[out_rows(s)],
            p2_s.at[s, o - 1],
            p2_r.at[s, o - 1],
            (d, q),
        )

    def own_copy(s):
        return pltpu.make_async_copy(tx2.at[s, z], out_hbm.at[out_rows(s)], own_sem.at[s])

    @pl.loop(0, steps)
    def _(s):
        for c in range(n_part):
            for o in range(1, n_col):
                p1_copy(c, s, o).wait_recv()

        @pl.loop(0, halves)
        def _(h):
            k = s * halves + h
            mixed = rx[s, pl.ds(pl.multiple_of(h * r_out, r_out), r_out), :]
            power = jnp.zeros((r_out, 1), jnp.float32)
            active = []
            for j in range(n_col):
                y = jnp.dot(
                    mixed, wfull[j].reshape(f_total, width), preferred_element_type=jnp.float32
                )
                y = jnp.maximum(y + bfull[j][0:1, :].astype(jnp.float32), 0.0)
                power = power + jnp.sum(y * y, axis=1, keepdims=True)
                active.append(y)
            factor = lax.rsqrt(power / f_total + epsilon)
            for j in range(n_col):
                scaled = active[j] * factor
                tx2[k, j] = scaled.astype(jnp.bfloat16)
                grouped = scaled.reshape(r_out // 8, 8, width)
                acc[j, 0] += jnp.sum(grouped, axis=0)
                acc[j, 1] += jnp.sum(grouped * grouped, axis=0)
            for o in range(1, n_col):
                p2_copy(k, o).start()
            own_copy(k).start()

    for j in range(n_col):
        part[j] = jnp.concatenate(
            [
                jnp.sum(acc[j, 0], axis=0, keepdims=True),
                jnp.sum(acc[j, 1], axis=0, keepdims=True),
                jnp.zeros((6, width), jnp.float32),
            ],
            axis=0,
        )

    def sd_copy(o):
        return remote(part, part_in.at[o], sd_s.at[o], sd_r.at[o], (lax.rem(d + o, n_dom), z))

    @pl.loop(1, n_dom)
    def _(o):
        sd_copy(o).start()

    part_in[0] = part[...]

    @pl.loop(1, n_dom)
    def _(o):
        sd_copy(o).wait()

    colpart[...] = jnp.sum(part_in[...], axis=0)

    def sc_copy(o):
        q = lax.rem(z + o, n_col)
        return remote(colpart.at[q], colpart_in.at[o], sc_s.at[o - 1], sc_r.at[o - 1], (d, q))

    for o in range(1, n_col):
        sc_copy(o).start()
    colpart_in[0] = colpart[z]

    for o in range(1, n_col):
        w_copy(o).wait_send()

    @pl.loop(1, n_dom)
    def _(o):
        w_pass(o).wait_send()
        for c in range(n_part):
            halo_arrived(c, lax.rem(d + o, n_dom)).wait_send()

    @pl.loop(0, steps)
    def _(s):
        for c in range(n_part):
            for o in range(1, n_col):
                p1_copy(c, s, o).wait_send()

    for o in range(1, n_col):
        sc_copy(o).wait()
    totals = jnp.sum(colpart_in[...], axis=0) / node_total
    mean = totals[0:1, :]
    stat_ref[...] = jnp.concatenate([mean, totals[1:2, :] - mean * mean], axis=0)

    @pl.loop(0, steps * halves)
    def _(s):
        for o in range(1, n_col):
            p2_copy(s, o).wait()
        own_copy(s).wait()


def on_device(
    features,
    weight,
    out_bias,
    local_index,
    local_count,
    local_vals,
    halo_index,
    halo_count,
    halo_vals,
    send_rows,
    send_count,
):
    rows, width = features.shape
    n_dom = lax.axis_size("dom")
    n_col = lax.axis_size("col")
    slot_total = send_rows.shape[2]
    f_total = weight.shape[0]
    n_part = width // LANES
    steps = rows // TILE // n_col // P1_TILES
    steps_out = rows // TILE // n_col // P2_TILES
    r_chunk = P1_TILES * TILE
    r_out = P2_TILES * TILE
    pieces = 8 if rows // TILE % 8 == 0 else 1
    any_spec = pl.BlockSpec(memory_space=pl.ANY)
    vmem = pl.BlockSpec(memory_space=pltpu.VMEM)
    smem = pl.BlockSpec(memory_space=pltpu.SMEM)
    bf16, f32 = jnp.bfloat16, jnp.float32
    dma = pltpu.SemaphoreType.DMA
    halo_bytes = 4 * n_dom * slot_total * width
    grant = 44 * 2**20 + 2 * halo_bytes
    held = pltpu.VMEM if grant + 2 * rows * width < 58 * 2**20 else jax.ShapeDtypeStruct
    grant = grant if held is pltpu.VMEM else 67043328
    normalized, stats = pl.pallas_call(
        functools.partial(kernel, n_dom, n_col, rows * n_dom),
        out_shape=(
            held((rows, width), bf16),
            held((2, width), f32),
        ),
        in_specs=[any_spec, any_spec, vmem, smem, smem, any_spec, smem, smem, any_spec, smem, smem],
        out_specs=(any_spec, vmem),
        scratch_shapes=[
            pltpu.VMEM((n_part, rows // TILE, TILE, LANES), bf16),
            pltpu.VMEM((n_part, rows, LANES), f32),
            pltpu.VMEM((slot_total, LANES), f32),
            pltpu.VMEM((n_part, n_dom, slot_total // TILE, TILE, LANES), bf16),
            pltpu.VMEM((n_dom * slot_total // TILE, TILE, LANES), bf16),
            pltpu.VMEM((n_dom * slot_total // TILE, TILE, LANES), bf16),
            pltpu.VMEM(local_vals.shape[1:], bf16),
            pltpu.VMEM(halo_vals.shape[1:], bf16),
            pltpu.VMEM((n_col, n_dom, f_total // n_dom, width), bf16),
            pltpu.VMEM((n_col, 16, width), bf16),
            pltpu.VMEM((n_part, steps, n_col - 1, r_chunk, LANES), bf16),
            pltpu.VMEM((steps, r_chunk, n_col * width), bf16),
            pltpu.VMEM((steps_out, n_col, r_out, width), bf16),
            pltpu.VMEM((n_col, 2, 8, width), f32),
            pltpu.VMEM((n_col, 8, width), f32),
            pltpu.VMEM((n_dom, n_col, 8, width), f32),
            pltpu.VMEM((n_col, 8, width), f32),
            pltpu.VMEM((n_col, 8, width), f32),
            dma((n_part, pieces)),
            dma((2,)),
            dma,
            dma((n_part, n_dom)),
            dma((n_part, n_dom)),
            dma((n_col - 1,)),
            dma((n_col - 1,)),
            dma((n_dom,)),
            dma((n_dom,)),
            dma((n_col - 1,)),
            dma((n_col - 1,)),
            dma((n_part, steps, n_col - 1)),
            dma((n_part, steps, n_col - 1)),
            dma((steps_out, n_col - 1)),
            dma((steps_out, n_col - 1)),
            dma((steps_out,)),
            dma((n_dom,)),
            dma((n_dom,)),
            dma((n_col - 1,)),
            dma((n_col - 1,)),
        ],
        compiler_params=pltpu.CompilerParams(
            collective_id=0, has_side_effects=True, vmem_limit_bytes=grant
        ),
    )(
        features.reshape(rows // TILE, TILE, width),
        weight,
        out_bias.reshape(1, width),
        local_index[0].T,
        local_count,
        local_vals[0],
        halo_index[0].T,
        halo_count,
        halo_vals[0],
        send_rows[0],
        send_count,
    )
    return normalized, stats


def solution(mesh):
    in_specs = (
        P("dom", "col"),
        P(None, "col"),
        P("col"),
        P("dom", None, None),
        P("dom", None),
        P("dom", None, None, None, None),
        P("dom", None, None),
        P("dom", None),
        P("dom", None, None, None, None),
        P("dom", None, None),
        P("dom", None),
    )
    out_specs = (P("dom", "col"), P(None, "col"))
    return jax.shard_map(
        on_device, mesh=mesh, in_specs=in_specs, out_specs=out_specs, check_vma=False
    )
```

```python
import functools

import jax
import jax.numpy as jnp
from jax import lax
from jax.experimental import pallas as pl
from jax.experimental.pallas import tpu as pltpu
from jax.sharding import PartitionSpec as P

TILE = 128
MESH = pl.DeviceIdType.MESH
LANES = 128
P1_TILES = 4
P2_TILES = 2
epsilon = 1e-06


def remote(src, dst, send_sem, recv_sem, device):
    return pltpu.make_async_remote_copy(
        src_ref=src,
        dst_ref=dst,
        send_sem=send_sem,
        recv_sem=recv_sem,
        device_id=device,
        device_id_type=MESH,
    )


def kernel(
    n_dom,
    n_col,
    node_total,
    feat_hbm,
    weight_hbm,
    bias_ref,
    lidx,
    lcnt,
    lvals_hbm,
    hidx,
    hcnt,
    hvals_hbm,
    srows,
    scnt,
    out_hbm,
    stat_ref,
    xb,
    xf,
    stage,
    outgoing,
    halo_a,
    halo_b,
    lvals,
    hvals,
    wfull,
    bfull,
    tx,
    rx,
    tx2,
    acc,
    part,
    part_in,
    colpart,
    colpart_in,
    feat_sem,
    vals_sem,
    wl_sem,
    halo_s,
    halo_r,
    w_s,
    w_r,
    wp_s,
    wp_r,
    b_s,
    b_r,
    p1_s,
    p1_r,
    p2_s,
    p2_r,
    own_sem,
    sd_s,
    sd_r,
    sc_s,
    sc_r,
):
    d = lax.axis_index("dom")
    z = lax.axis_index("col")
    halos = (halo_a, halo_b)
    n_part, rows, lanes = xf.shape
    width = n_part * lanes
    slot_total = srows.shape[1]
    k_local = lvals.shape[1]
    k_halo = hvals.shape[1]
    f_total = weight_hbm.shape[0]
    tiles_q = rows // TILE // n_col
    rows_q = tiles_q * TILE
    ct = P1_TILES
    r_chunk = ct * TILE
    steps = tiles_q // ct
    r_out = P2_TILES * TILE
    halves = r_chunk // r_out
    per_peer = slot_total // TILE
    shard = f_total // n_dom
    n_chips = n_dom // 2
    chip = d // 2
    core = lax.rem(d, 2)
    mate = d + 1 - 2 * core

    pieces = feat_sem.shape[1]
    piece = rows // TILE // pieces

    def feat_copy(c, i):
        at = pl.ds(i * piece, piece)
        return pltpu.make_async_copy(
            feat_hbm.at[at, :, pl.ds(c * lanes, lanes)], xb.at[c, at], feat_sem.at[c, i]
        )

    def w_load():
        mine = pl.ds(pl.multiple_of(d * shard, shard), shard)
        return pltpu.make_async_copy(weight_hbm.at[mine], wfull.at[z, d], wl_sem)

    for i in range(pieces):
        feat_copy(0, i).start()
    w_load().start()
    for i in range(pieces):
        feat_copy(1, i).start()
    bfull[z] = jnp.broadcast_to(bias_ref[...].reshape(1, width), bfull.shape[1:])

    barrier = pltpu.get_barrier_semaphore()
    for o in range(1, n_dom):
        pl.semaphore_signal(barrier, inc=1, device_id=(lax.rem(d + o, n_dom), z), device_id_type=MESH)
    for o in range(1, n_col):
        pl.semaphore_signal(barrier, inc=1, device_id=(d, lax.rem(z + o, n_col)), device_id_type=MESH)

    def widen(c):
        @pl.loop(0, pieces)
        def _(i):
            feat_copy(c, i).wait()
            for j in range(piece):
                t = i * piece + j
                xf[c, pl.ds(pl.multiple_of(t * TILE, TILE), TILE), :] = xb[c, t].astype(jnp.float32)

    widen(0)
    lv_copy = pltpu.make_async_copy(lvals_hbm, lvals, vals_sem.at[0])
    hv_copy = pltpu.make_async_copy(hvals_hbm, hvals, vals_sem.at[1])
    lv_copy.start()
    hv_copy.start()
    pl.semaphore_wait(barrier, n_dom - 1 + n_col - 1)

    def w_copy(o):
        return remote(
            wfull.at[z, d], wfull.at[z, d], w_s.at[o - 1], w_r.at[o - 1], (d, lax.rem(z + o, n_col))
        )

    def w_arrived(o):
        src = lax.rem(z + n_col - o, n_col)
        return remote(
            wfull.at[src, d], wfull.at[src, d], w_s.at[o - 1], w_r.at[o - 1], (d, src)
        )

    def w_pass(o):
        return remote(
            wfull.at[:, d], wfull.at[:, d], wp_s.at[o], wp_r.at[o], (lax.rem(d + o, n_dom), z)
        )

    def w_passed(o):
        src = lax.rem(d + n_dom - o, n_dom)
        return remote(wfull.at[:, src], wfull.at[:, src], wp_s.at[o], wp_r.at[o], (src, z))

    def b_copy(o):
        return remote(
            bfull.at[z], bfull.at[z], b_s.at[o - 1], b_r.at[o - 1], (d, lax.rem(z + o, n_col))
        )

    w_load().wait()
    for o in range(1, n_col):
        w_copy(o).start()
        b_copy(o).start()

    def slots_of(q):
        return pl.ds(q * per_peer, per_peer)

    def halo_send(c, peer):
        return remote(
            outgoing.at[c, peer],
            halos[c].at[slots_of(d)],
            halo_s.at[c, peer],
            halo_r.at[c, d],
            (peer, z),
        )

    def halo_arrived(c, src):
        return remote(
            outgoing.at[c, src],
            halos[c].at[slots_of(src)],
            halo_s.at[c, src],
            halo_r.at[c, src],
            (src, z),
        )

    def gather(c, peer):
        @pl.loop(0, slot_total // LANES)
        def _(g):
            group = pl.ds(pl.multiple_of(g * LANES, LANES), LANES)
            picked = srows.at[:, group]
            into = stage.at[group]
            for k in range(LANES):
                into[k] = xf[c, picked[peer, k]]

        used = lax.broadcasted_iota(jnp.int32, (slot_total, lanes), 0) < scnt[0, peer]
        sent = jnp.where(used, stage[...], 0.0).astype(outgoing.dtype)
        outgoing[c, peer] = sent.reshape(per_peer, TILE, lanes)
        halo_send(c, peer).start()

    def gather_all(c):
        @pl.loop(0, n_dom - 1)
        def _(i):
            side = i // n_chips
            at_mate = (i + 1) // n_chips - side
            over = 2 * lax.rem(chip + lax.rem(i, n_chips) + 1, n_chips) + side
            gather(c, over + at_mate * (1 - core))

    def zero_own(c):
        halos[c][slots_of(d)] = jnp.zeros((per_peer, TILE, lanes), halo_a.dtype)

    gather_all(0)
    widen(1)
    for c in range(n_part):
        zero_own(c)

    @pl.when(core == 1)
    def _():
        gather_all(1)

    lv_copy.wait()
    hv_copy.wait()

    def kept(count, k):
        one = jnp.minimum(jnp.maximum(count - k, 0), 1).astype(jnp.float32)
        return jnp.broadcast_to(one, (TILE, TILE)).astype(jnp.bfloat16)

    def tile_rows(c, t):
        lhs, rhs = [], []
        n_loc, n_hal = lcnt[0, t], hcnt[0, t]
        for k in range(k_local):
            lhs.append(lvals[t, k] * kept(n_loc, k))
            rhs.append(xb[c, lidx[k, t]])
        for k in range(k_halo):
            lhs.append(hvals[t, k] * kept(n_hal, k))
            rhs.append(halos[c][hidx[k, t]])
        total = jnp.dot(
            jnp.concatenate(lhs, axis=1),
            jnp.concatenate(rhs, axis=0),
            preferred_element_type=jnp.float32,
        )
        return total.astype(jnp.bfloat16)

    def my_cols(c):
        return pl.ds(pl.multiple_of(z * width + c * lanes, lanes), lanes)

    def p1_copy(c, s, o):
        return remote(
            tx.at[c, s, o - 1],
            rx.at[s, :, my_cols(c)],
            p1_s.at[c, s, o - 1],
            p1_r.at[c, s, o - 1],
            (d, lax.rem(z + o, n_col)),
        )

    for c in range(n_part):

        @pl.loop(1, n_dom)
        def _(o):
            halo_arrived(c, lax.rem(d + o, n_dom)).wait_recv()

        @pl.loop(0, steps)
        def _(s):
            for o in range(1, n_col):
                q = lax.rem(z + o, n_col)
                for i in range(ct):
                    tx[c, s, o - 1, i * TILE : (i + 1) * TILE, :] = tile_rows(c, q * tiles_q + s * ct + i)
                p1_copy(c, s, o).start()
            for i in range(ct):
                rx[s, i * TILE : (i + 1) * TILE, my_cols(c)] = tile_rows(c, z * tiles_q + s * ct + i)

        if c == 0:

            @pl.when(core == 0)
            def _():
                gather_all(1)

            for o in range(1, n_col):
                w_arrived(o).wait_recv()

            @pl.loop(1, n_dom)
            def _(o):
                w_pass(o).start()

    @pl.loop(1, n_dom)
    def _(o):
        w_passed(o).wait_recv()

    for o in range(1, n_col):
        b_copy(o).wait()

    acc[...] = jnp.zeros_like(acc)

    def out_rows(s):
        return pl.ds(pl.multiple_of(z * rows_q + s * r_out, r_out), r_out)

    def p2_copy(s, o):
        q = lax.rem(z + o, n_col)
        return remote(
            tx2.at[s, q],
            out_hbm.at[out_rows(s)],
            p2_s.at[s, o - 1],
            p2_r.at[s, o - 1],
            (d, q),
        )

    def own_copy(s):
        return pltpu.make_async_copy(tx2.at[s, z], out_hbm.at[out_rows(s)], own_sem.at[s])

    @pl.loop(0, steps)
    def _(s):
        for c in range(n_part):
            for o in range(1, n_col):
                p1_copy(c, s, o).wait_recv()

        @pl.loop(0, halves)
        def _(h):
            k = s * halves + h
            mixed = rx[s, pl.ds(pl.multiple_of(h * r_out, r_out), r_out), :]
            power = jnp.zeros((r_out, 1), jnp.float32)
            active = []
            for j in range(n_col):
                y = jnp.dot(
                    mixed, wfull[j].reshape(f_total, width), preferred_element_type=jnp.float32
                )
                y = jnp.maximum(y + bfull[j][0:1, :].astype(jnp.float32), 0.0)
                power = power + jnp.sum(y * y, axis=1, keepdims=True)
                active.append(y)
            factor = lax.rsqrt(power / f_total + epsilon)
            for j in range(n_col):
                scaled = active[j] * factor
                tx2[k, j] = scaled.astype(jnp.bfloat16)
                grouped = scaled.reshape(r_out // 8, 8, width)
                acc[j, 0] += jnp.sum(grouped, axis=0)
                acc[j, 1] += jnp.sum(grouped * grouped, axis=0)
            for o in range(1, n_col):
                p2_copy(k, o).start()
            own_copy(k).start()

    for j in range(n_col):
        part[j] = jnp.concatenate(
            [
                jnp.sum(acc[j, 0], axis=0, keepdims=True),
                jnp.sum(acc[j, 1], axis=0, keepdims=True),
                jnp.zeros((6, width), jnp.float32),
            ],
            axis=0,
        )

    def sd_copy(o):
        return remote(part, part_in.at[o], sd_s.at[o], sd_r.at[o], (lax.rem(d + o, n_dom), z))

    @pl.loop(1, n_dom)
    def _(o):
        sd_copy(o).start()

    part_in[0] = part[...]

    @pl.loop(1, n_dom)
    def _(o):
        sd_copy(o).wait()

    colpart[...] = jnp.sum(part_in[...], axis=0)

    def sc_copy(o):
        q = lax.rem(z + o, n_col)
        return remote(colpart.at[q], colpart_in.at[o], sc_s.at[o - 1], sc_r.at[o - 1], (d, q))

    for o in range(1, n_col):
        sc_copy(o).start()
    colpart_in[0] = colpart[z]

    for o in range(1, n_col):
        w_copy(o).wait_send()

    @pl.loop(1, n_dom)
    def _(o):
        w_pass(o).wait_send()
        for c in range(n_part):
            halo_arrived(c, lax.rem(d + o, n_dom)).wait_send()

    @pl.loop(0, steps)
    def _(s):
        for c in range(n_part):
            for o in range(1, n_col):
                p1_copy(c, s, o).wait_send()

    for o in range(1, n_col):
        sc_copy(o).wait()
    totals = jnp.sum(colpart_in[...], axis=0) / node_total
    mean = totals[0:1, :]
    stat_ref[...] = jnp.concatenate([mean, totals[1:2, :] - mean * mean], axis=0)

    @pl.loop(0, steps * halves)
    def _(s):
        for o in range(1, n_col):
            p2_copy(s, o).wait()
        own_copy(s).wait()


def on_device(
    features,
    weight,
    out_bias,
    local_index,
    local_count,
    local_vals,
    halo_index,
    halo_count,
    halo_vals,
    send_rows,
    send_count,
):
    rows, width = features.shape
    n_dom = lax.axis_size("dom")
    n_col = lax.axis_size("col")
    slot_total = send_rows.shape[2]
    f_total = weight.shape[0]
    n_part = width // LANES
    steps = rows // TILE // n_col // P1_TILES
    steps_out = rows // TILE // n_col // P2_TILES
    r_chunk = P1_TILES * TILE
    r_out = P2_TILES * TILE
    pieces = 8 if rows // TILE % 8 == 0 else 1
    any_spec = pl.BlockSpec(memory_space=pl.ANY)
    vmem = pl.BlockSpec(memory_space=pltpu.VMEM)
    smem = pl.BlockSpec(memory_space=pltpu.SMEM)
    bf16, f32 = jnp.bfloat16, jnp.float32
    dma = pltpu.SemaphoreType.DMA
    halo_bytes = 4 * n_dom * slot_total * width
    grant = 44 * 2**20 + 2 * halo_bytes
    held = pltpu.VMEM if grant + 2 * rows * width < 58 * 2**20 else jax.ShapeDtypeStruct
    grant = grant if held is pltpu.VMEM else 67043328
    normalized, stats = pl.pallas_call(
        functools.partial(kernel, n_dom, n_col, rows * n_dom),
        out_shape=(
            held((rows, width), bf16),
            held((2, width), f32),
        ),
        in_specs=[any_spec, any_spec, vmem, smem, smem, any_spec, smem, smem, any_spec, smem, smem],
        out_specs=(any_spec, vmem),
        scratch_shapes=[
            pltpu.VMEM((n_part, rows // TILE, TILE, LANES), bf16),
            pltpu.VMEM((n_part, rows, LANES), f32),
            pltpu.VMEM((slot_total, LANES), f32),
            pltpu.VMEM((n_part, n_dom, slot_total // TILE, TILE, LANES), bf16),
            pltpu.VMEM((n_dom * slot_total // TILE, TILE, LANES), bf16),
            pltpu.VMEM((n_dom * slot_total // TILE, TILE, LANES), bf16),
            pltpu.VMEM(local_vals.shape[1:], bf16),
            pltpu.VMEM(halo_vals.shape[1:], bf16),
            pltpu.VMEM((n_col, n_dom, f_total // n_dom, width), bf16),
            pltpu.VMEM((n_col, 16, width), bf16),
            pltpu.VMEM((n_part, steps, n_col - 1, r_chunk, LANES), bf16),
            pltpu.VMEM((steps, r_chunk, n_col * width), bf16),
            pltpu.VMEM((steps_out, n_col, r_out, width), bf16),
            pltpu.VMEM((n_col, 2, 8, width), f32),
            pltpu.VMEM((n_col, 8, width), f32),
            pltpu.VMEM((n_dom, n_col, 8, width), f32),
            pltpu.VMEM((n_col, 8, width), f32),
            pltpu.VMEM((n_col, 8, width), f32),
            dma((n_part, pieces)),
            dma((2,)),
            dma,
            dma((n_part, n_dom)),
            dma((n_part, n_dom)),
            dma((n_col - 1,)),
            dma((n_col - 1,)),
            dma((n_dom,)),
            dma((n_dom,)),
            dma((n_col - 1,)),
            dma((n_col - 1,)),
            dma((n_part, steps, n_col - 1)),
            dma((n_part, steps, n_col - 1)),
            dma((steps_out, n_col - 1)),
            dma((steps_out, n_col - 1)),
            dma((steps_out,)),
            dma((n_dom,)),
            dma((n_dom,)),
            dma((n_col - 1,)),
            dma((n_col - 1,)),
        ],
        compiler_params=pltpu.CompilerParams(
            collective_id=0, has_side_effects=True, vmem_limit_bytes=grant
        ),
    )(
        features.reshape(rows // TILE, TILE, width),
        weight,
        out_bias,
        local_index[0].T,
        local_count,
        local_vals[0],
        halo_index[0].T,
        halo_count,
        halo_vals[0],
        send_rows[0],
        send_count,
    )
    return normalized, stats


def solution(mesh):
    in_specs = (
        P("dom", "col"),
        P(None, "col"),
        P("col"),
        P("dom", None, None),
        P("dom", None),
        P("dom", None, None, None, None),
        P("dom", None, None),
        P("dom", None),
        P("dom", None, None, None, None),
        P("dom", None, None),
        P("dom", None),
    )
    out_specs = (P("dom", "col"), P(None, "col"))
    return jax.shard_map(
        on_device, mesh=mesh, in_specs=in_specs, out_specs=out_specs, check_vma=False
    )
```

```python
import functools

import jax
import jax.numpy as jnp
from jax import lax
from jax.experimental import pallas as pl
from jax.experimental.pallas import tpu as pltpu
from jax.sharding import PartitionSpec as P

TILE = 128
MESH = pl.DeviceIdType.MESH
LANES = 128
P1_TILES = 4
P2_TILES = 2
epsilon = 1e-06


def remote(src, dst, send_sem, recv_sem, device):
    return pltpu.make_async_remote_copy(
        src_ref=src,
        dst_ref=dst,
        send_sem=send_sem,
        recv_sem=recv_sem,
        device_id=device,
        device_id_type=MESH,
    )


def kernel(
    n_dom,
    n_col,
    node_total,
    feat_hbm,
    weight_hbm,
    bias_ref,
    lidx_hbm,
    lcnt_hbm,
    lvals_hbm,
    hidx_hbm,
    hcnt_hbm,
    hvals_hbm,
    srows_hbm,
    scnt_hbm,
    out_hbm,
    stat_ref,
    xb,
    xf,
    stage,
    outgoing,
    halo_a,
    halo_b,
    lvals,
    hvals,
    wfull,
    bfull,
    tx,
    rx,
    tx2,
    acc,
    part,
    part_in,
    colpart,
    colpart_in,
    lidx,
    lcnt,
    hidx,
    hcnt,
    srows,
    scnt,
    feat_sem,
    late_sem,
    index_sem,
    vals_sem,
    wl_sem,
    halo_s,
    halo_r,
    w_s,
    w_r,
    wp_s,
    wp_r,
    b_s,
    b_r,
    p1_s,
    p1_r,
    p2_s,
    p2_r,
    own_sem,
    sd_s,
    sd_r,
    sc_s,
    sc_r,
):
    d = lax.axis_index("dom")
    z = lax.axis_index("col")
    halos = (halo_a, halo_b)
    n_part, rows, lanes = xf.shape
    width = n_part * lanes
    slot_total = srows.shape[1]
    k_local = lvals.shape[1]
    k_halo = hvals.shape[1]
    f_total = weight_hbm.shape[0]
    tiles_q = rows // TILE // n_col
    rows_q = tiles_q * TILE
    ct = P1_TILES
    r_chunk = ct * TILE
    steps = tiles_q // ct
    r_out = P2_TILES * TILE
    halves = r_chunk // r_out
    per_peer = slot_total // TILE
    shard = f_total // n_dom
    n_chips = n_dom // 2
    chip = d // 2
    core = lax.rem(d, 2)
    mate = d + 1 - 2 * core

    pieces = feat_sem.shape[0]
    piece = rows // TILE // pieces

    def feat_copy(i):
        at = pl.ds(i * piece, piece)
        return pltpu.make_async_copy(
            feat_hbm.at[at, :, pl.ds(0, lanes)], xb.at[0, at], feat_sem.at[i]
        )

    def late_copy():
        return pltpu.make_async_copy(
            feat_hbm.at[:, :, pl.ds(lanes, lanes)], xb.at[1], late_sem
        )

    tables = [
        pltpu.make_async_copy(src, dst, index_sem.at[i])
        for i, (src, dst) in enumerate(
            (
                (srows_hbm, srows),
                (scnt_hbm, scnt),
                (lidx_hbm, lidx),
                (lcnt_hbm, lcnt),
                (hidx_hbm, hidx),
                (hcnt_hbm, hcnt),
            )
        )
    ]

    def w_load():
        mine = pl.ds(pl.multiple_of(d * shard, shard), shard)
        return pltpu.make_async_copy(weight_hbm.at[mine], wfull.at[z, d], wl_sem)

    for copy in tables[:2]:
        copy.start()
    for i in range(pieces):
        feat_copy(i).start()
    w_load().start()
    late_copy().start()
    for copy in tables[2:]:
        copy.start()

    barrier = pltpu.get_barrier_semaphore()
    for o in range(1, n_dom):
        pl.semaphore_signal(barrier, inc=1, device_id=(lax.rem(d + o, n_dom), z), device_id_type=MESH)
    for o in range(1, n_col):
        pl.semaphore_signal(barrier, inc=1, device_id=(d, lax.rem(z + o, n_col)), device_id_type=MESH)
    bfull[z] = jnp.broadcast_to(bias_ref[...].reshape(1, width), bfull.shape[1:])

    def widen(c, t):
        xf[c, pl.ds(pl.multiple_of(t * TILE, TILE), TILE), :] = xb[c, t].astype(jnp.float32)

    @pl.loop(0, pieces)
    def _(i):
        feat_copy(i).wait()
        for j in range(piece):
            widen(0, i * piece + j)

    def widen_late():
        late_copy().wait()

        @pl.loop(0, pieces)
        def _(i):
            for j in range(piece):
                widen(1, i * piece + j)

    def peer_of(i):
        side = i // n_chips
        at_mate = (i + 1) // n_chips - side
        over = 2 * lax.rem(chip + lax.rem(i, n_chips) + 1, n_chips) + side
        return over + at_mate * (1 - core)

    def slots_of(q):
        return pl.ds(q * per_peer, per_peer)

    def halo_send(c, peer):
        return remote(
            outgoing.at[c, peer],
            halos[c].at[slots_of(d)],
            halo_s.at[c],
            halo_r.at[c],
            (peer, z),
        )

    def halo_all(c):
        most = pl.ds(0, n_dom - 1)
        return remote(
            outgoing.at[c, most],
            outgoing.at[c, most],
            halo_s.at[c],
            halo_r.at[c],
            (mate, z),
        )

    def gather(c, peer):
        @pl.loop(0, slot_total // LANES)
        def _(g):
            group = pl.ds(pl.multiple_of(g * LANES, LANES), LANES)
            picked = srows.at[:, group]
            into = stage.at[group]
            for k in range(LANES):
                into[k] = xf[c, picked[peer, k]]

        used = lax.broadcasted_iota(jnp.int32, (slot_total, lanes), 0) < scnt[0, peer]
        sent = jnp.where(used, stage[...], 0.0).astype(outgoing.dtype)
        outgoing[c, peer] = sent.reshape(per_peer, TILE, lanes)

    def gather_all(c, first):
        @pl.loop(first, n_dom - 1)
        def _(i):
            gather(c, peer_of(i))
            halo_send(c, peer_of(i)).start()

    for copy in tables[:2]:
        copy.wait()
    gather(0, peer_of(0))
    lv_copy = pltpu.make_async_copy(lvals_hbm, lvals, vals_sem.at[0])
    hv_copy = pltpu.make_async_copy(hvals_hbm, hvals, vals_sem.at[1])
    lv_copy.start()
    hv_copy.start()
    pl.semaphore_wait(barrier, n_dom - 1 + n_col - 1)
    halo_send(0, peer_of(0)).start()

    def w_copy(o):
        return remote(wfull.at[z, d], wfull.at[z, d], w_s, w_r, (d, lax.rem(z + o, n_col)))

    def w_copies():
        some = pl.ds(0, n_col - 1)
        return remote(wfull.at[some, d], wfull.at[some, d], w_s, w_r, (d, lax.rem(z + 1, n_col)))

    def w_pass(o):
        return remote(wfull.at[:, d], wfull.at[:, d], wp_s, wp_r, (lax.rem(d + o, n_dom), z))

    def w_passes():
        most = pl.ds(0, n_dom - 1)
        return remote(wfull.at[:, most], wfull.at[:, most], wp_s, wp_r, (mate, z))

    def b_copy(o):
        return remote(bfull.at[z], bfull.at[z], b_s, b_r, (d, lax.rem(z + o, n_col)))

    def b_copies():
        some = bfull.at[pl.ds(0, n_col - 1)]
        return remote(some, some, b_s, b_r, (d, lax.rem(z + 1, n_col)))

    w_load().wait()
    for o in range(1, n_col):
        w_copy(o).start()
        b_copy(o).start()

    def zero_own(c):
        halos[c][slots_of(d)] = jnp.zeros((per_peer, TILE, lanes), halo_a.dtype)

    gather_all(0, 1)
    widen_late()
    for c in range(n_part):
        zero_own(c)

    @pl.when(core == 1)
    def _():
        gather_all(1, 0)

    for copy in tables[2:]:
        copy.wait()
    lv_copy.wait()
    hv_copy.wait()

    def kept(count, k):
        one = jnp.minimum(jnp.maximum(count - k, 0), 1).astype(jnp.float32)
        return jnp.broadcast_to(one, (TILE, TILE)).astype(jnp.bfloat16)

    def tile_rows(c, t):
        lhs, rhs = [], []
        n_loc, n_hal = lcnt[0, t], hcnt[0, t]
        for k in range(k_local):
            lhs.append(lvals[t, k] * kept(n_loc, k))
            rhs.append(xb[c, lidx[k, t]])
        for k in range(k_halo):
            lhs.append(hvals[t, k] * kept(n_hal, k))
            rhs.append(halos[c][hidx[k, t]])
        total = jnp.dot(
            jnp.concatenate(lhs, axis=1),
            jnp.concatenate(rhs, axis=0),
            preferred_element_type=jnp.float32,
        )
        return total.astype(jnp.bfloat16)

    def p1_copy(c, s, o):
        return remote(
            tx.at[s, o - 1, c], rx.at[s, z, c], p1_s, p1_r.at[s], (d, lax.rem(z + o, n_col))
        )

    def p1_step(s):
        whole = tx.at[s]
        return remote(whole, whole, p1_s, p1_r.at[s], (d, lax.rem(z + 1, n_col)))

    for c in range(n_part):

        halo_all(c).wait_recv()

        @pl.loop(0, steps)
        def _(s):
            for o in range(1, n_col):
                q = lax.rem(z + o, n_col)
                for i in range(ct):
                    tx[s, o - 1, c, i * TILE : (i + 1) * TILE, :] = tile_rows(c, q * tiles_q + s * ct + i)
                p1_copy(c, s, o).start()
            for i in range(ct):
                rx[s, z, c, i * TILE : (i + 1) * TILE, :] = tile_rows(c, z * tiles_q + s * ct + i)

        if c == 0:

            @pl.when(core == 0)
            def _():
                gather_all(1, 0)

            w_copies().wait_recv()

            @pl.loop(1, n_dom)
            def _(o):
                w_pass(o).start()

    w_passes().wait_recv()
    b_copies().wait()

    acc[...] = jnp.zeros_like(acc)

    def out_rows(s):
        return pl.ds(pl.multiple_of(z * rows_q + s * r_out, r_out), r_out)

    def p2_copy(s, o):
        q = lax.rem(z + o, n_col)
        return remote(tx2.at[s, q], out_hbm.at[out_rows(s)], p2_s, p2_r, (d, q))

    def p2_all():
        most = tx2.at[:, pl.ds(0, n_col - 1)]
        return remote(most, most, p2_s, p2_r, (d, lax.rem(z + 1, n_col)))

    def own_copy(s):
        return pltpu.make_async_copy(tx2.at[s, z], out_hbm.at[out_rows(s)], own_sem)

    def own_all():
        mine = tx2.at[:, z]
        return pltpu.make_async_copy(mine, mine, own_sem)

    @pl.loop(0, steps)
    def _(s):
        p1_step(s).wait_recv()

        @pl.loop(0, halves)
        def _(h):
            k = s * halves + h
            at = pl.ds(pl.multiple_of(h * r_out, r_out), r_out)
            mixed = jnp.concatenate(
                [rx[s, j, c, at, :] for j in range(n_col) for c in range(n_part)], axis=1
            )
            power = jnp.zeros((r_out, 1), jnp.float32)
            active = []
            for j in range(n_col):
                y = jnp.dot(
                    mixed, wfull[j].reshape(f_total, width), preferred_element_type=jnp.float32
                )
                y = jnp.maximum(y + bfull[j][0:1, :].astype(jnp.float32), 0.0)
                power = power + jnp.sum(y * y, axis=1, keepdims=True)
                active.append(y)
            factor = lax.rsqrt(power / f_total + epsilon)
            for j in range(n_col):
                scaled = active[j] * factor
                tx2[k, j] = scaled.astype(jnp.bfloat16)
                grouped = scaled.reshape(r_out // 8, 8, width)
                acc[j, 0] += jnp.sum(grouped, axis=0)
                acc[j, 1] += jnp.sum(grouped * grouped, axis=0)
            for o in range(1, n_col):
                p2_copy(k, o).start()
            own_copy(k).start()

    for j in range(n_col):
        part[j] = jnp.concatenate(
            [
                jnp.sum(acc[j, 0], axis=0, keepdims=True),
                jnp.sum(acc[j, 1], axis=0, keepdims=True),
                jnp.zeros((6, width), jnp.float32),
            ],
            axis=0,
        )

    def sd_copy(o):
        return remote(part, part_in.at[o], sd_s, sd_r, (lax.rem(d + o, n_dom), z))

    def sd_all():
        most = part_in.at[pl.ds(1, n_dom - 1)]
        return remote(most, most, sd_s, sd_r, (mate, z))

    @pl.loop(1, n_dom)
    def _(o):
        sd_copy(o).start()

    part_in[0] = part[...]
    sd_all().wait()
    colpart[...] = jnp.sum(part_in[...], axis=0)

    def sc_copy(o):
        q = lax.rem(z + o, n_col)
        return remote(colpart.at[q], colpart_in.at[o], sc_s, sc_r, (d, q))

    def sc_all():
        some = colpart_in.at[pl.ds(1, n_col - 1)]
        return remote(some, some, sc_s, sc_r, (d, lax.rem(z + 1, n_col)))

    for o in range(1, n_col):
        sc_copy(o).start()
    colpart_in[0] = colpart[z]

    w_copies().wait_send()
    w_passes().wait_send()
    for c in range(n_part):
        halo_all(c).wait_send()

    remote(tx, tx, p1_s, p1_r.at[0], (d, lax.rem(z + 1, n_col))).wait_send()
    sc_all().wait()
    totals = jnp.sum(colpart_in[...], axis=0) / node_total
    mean = totals[0:1, :]
    stat_ref[...] = jnp.concatenate([mean, totals[1:2, :] - mean * mean], axis=0)

    p2_all().wait()
    own_all().wait()


def on_device(
    features,
    weight,
    out_bias,
    local_index,
    local_count,
    local_vals,
    halo_index,
    halo_count,
    halo_vals,
    send_rows,
    send_count,
):
    rows, width = features.shape
    n_dom = lax.axis_size("dom")
    n_col = lax.axis_size("col")
    slot_total = send_rows.shape[2]
    f_total = weight.shape[0]
    n_part = width // LANES
    steps = rows // TILE // n_col // P1_TILES
    steps_out = rows // TILE // n_col // P2_TILES
    r_chunk = P1_TILES * TILE
    r_out = P2_TILES * TILE
    pieces = 8 if rows // TILE % 8 == 0 else 1
    any_spec = pl.BlockSpec(memory_space=pl.ANY)
    vmem = pl.BlockSpec(memory_space=pltpu.VMEM)
    bf16, f32 = jnp.bfloat16, jnp.float32
    dma = pltpu.SemaphoreType.DMA

    def table(*shape):
        return pltpu.SMEM(shape, jnp.int32)

    halo_bytes = 4 * n_dom * slot_total * width
    grant = 44 * 2**20 + 2 * halo_bytes
    held = pltpu.VMEM if grant + 2 * rows * width < 58 * 2**20 else jax.ShapeDtypeStruct
    grant = grant if held is pltpu.VMEM else 67043328
    normalized, stats = pl.pallas_call(
        functools.partial(kernel, n_dom, n_col, rows * n_dom),
        out_shape=(
            held((rows, width), bf16),
            held((2, width), f32),
        ),
        in_specs=[any_spec, any_spec, vmem] + [any_spec] * 8,
        out_specs=(any_spec, vmem),
        scratch_shapes=[
            pltpu.VMEM((n_part, rows // TILE, TILE, LANES), bf16),
            pltpu.VMEM((n_part, rows, LANES), f32),
            pltpu.VMEM((slot_total, LANES), f32),
            pltpu.VMEM((n_part, n_dom, slot_total // TILE, TILE, LANES), bf16),
            pltpu.VMEM((n_dom * slot_total // TILE, TILE, LANES), bf16),
            pltpu.VMEM((n_dom * slot_total // TILE, TILE, LANES), bf16),
            pltpu.VMEM(local_vals.shape[1:], bf16),
            pltpu.VMEM(halo_vals.shape[1:], bf16),
            pltpu.VMEM((n_col, n_dom, f_total // n_dom, width), bf16),
            pltpu.VMEM((n_col, 16, width), bf16),
            pltpu.VMEM((steps, n_col - 1, n_part, r_chunk, LANES), bf16),
            pltpu.VMEM((steps, n_col, n_part, r_chunk, LANES), bf16),
            pltpu.VMEM((steps_out, n_col, r_out, width), bf16),
            pltpu.VMEM((n_col, 2, 8, width), f32),
            pltpu.VMEM((n_col, 8, width), f32),
            pltpu.VMEM((n_dom, n_col, 8, width), f32),
            pltpu.VMEM((n_col, 8, width), f32),
            pltpu.VMEM((n_col, 8, width), f32),
            table(local_index.shape[2], rows // TILE),
            table(1, rows // TILE),
            table(halo_index.shape[2], rows // TILE),
            table(1, rows // TILE),
            table(n_dom, slot_total),
            table(1, n_dom),
            dma((pieces,)),
            dma,
            dma((6,)),
            dma((2,)),
            dma,
            dma((n_part,)),
            dma((n_part,)),
            dma,
            dma,
            dma,
            dma,
            dma,
            dma,
            dma,
            dma((steps,)),
            dma,
            dma,
            dma,
            dma,
            dma,
            dma,
            dma,
        ],
        compiler_params=pltpu.CompilerParams(
            collective_id=0, has_side_effects=True, vmem_limit_bytes=grant
        ),
    )(
        features.reshape(rows // TILE, TILE, width),
        weight,
        out_bias,
        local_index[0].T,
        local_count,
        local_vals[0],
        halo_index[0].T,
        halo_count,
        halo_vals[0],
        send_rows[0],
        send_count,
    )
    return normalized, stats


def solution(mesh):
    in_specs = (
        P("dom", "col"),
        P(None, "col"),
        P("col"),
        P("dom", None, None),
        P("dom", None),
        P("dom", None, None, None, None),
        P("dom", None, None),
        P("dom", None),
        P("dom", None, None, None, None),
        P("dom", None, None),
        P("dom", None),
    )
    out_specs = (P("dom", "col"), P(None, "col"))
    return jax.shard_map(
        on_device, mesh=mesh, in_specs=in_specs, out_specs=out_specs, check_vma=False
    )
```

```python
import functools

import jax
import jax.numpy as jnp
from jax import lax
from jax.experimental import pallas as pl
from jax.experimental.pallas import tpu as pltpu
from jax.sharding import PartitionSpec as P

TILE = 128
MESH = pl.DeviceIdType.MESH
LANES = 128
P1_TILES = 4
P2_TILES = 2
EARLY_STEPS = 1
epsilon = 1e-06


def remote(src, dst, send_sem, recv_sem, device):
    return pltpu.make_async_remote_copy(
        src_ref=src,
        dst_ref=dst,
        send_sem=send_sem,
        recv_sem=recv_sem,
        device_id=device,
        device_id_type=MESH,
    )


def kernel(
    n_dom,
    n_col,
    node_total,
    feat_hbm,
    weight_hbm,
    bias_ref,
    lidx_hbm,
    lcnt_hbm,
    lvals_hbm,
    hidx_hbm,
    hcnt_hbm,
    hvals_hbm,
    srows_hbm,
    scnt_hbm,
    out_hbm,
    stat_ref,
    xb,
    xf,
    stage,
    out_a,
    out_b,
    out_late,
    land_a,
    land_b,
    halo_early,
    halo_late,
    lvals,
    hvals,
    wfull,
    bfull,
    tx,
    rx,
    tx2,
    acc,
    part,
    part_in,
    colpart,
    colpart_in,
    lidx,
    lcnt,
    hidx,
    hcnt,
    srows,
    scnt,
    feat_sem,
    late_sem,
    index_sem,
    vals_sem,
    wl_sem,
    halo_s,
    halo_r,
    w_s,
    w_r,
    wp_s,
    wp_r,
    b_s,
    b_r,
    p1_s,
    p1_r,
    p2_s,
    p2_r,
    own_sem,
    sd_s,
    sd_r,
    sc_s,
    sc_r,
):
    d = lax.axis_index("dom")
    z = lax.axis_index("col")
    halos = (halo_early, halo_late)
    outs = (out_a, out_b, out_late)
    lands = (land_a, land_b, halo_late)
    n_part, rows, lanes = xf.shape
    width = n_part * lanes
    slot_total = srows.shape[1]
    k_local = lvals.shape[1]
    k_halo = hvals.shape[1]
    f_total = weight_hbm.shape[0]
    tiles_q = rows // TILE // n_col
    rows_q = tiles_q * TILE
    ct = P1_TILES
    r_chunk = ct * TILE
    steps = tiles_q // ct
    r_out = P2_TILES * TILE
    halves = r_chunk // r_out
    per_peer = slot_total // TILE
    half_peer = per_peer // 2
    shard = f_total // n_dom
    n_chips = n_dom // 2
    chip = d // 2
    core = lax.rem(d, 2)
    mate = d + 1 - 2 * core

    pieces = feat_sem.shape[0]
    piece = rows // TILE // pieces

    def feat_copy(i):
        at = pl.ds(i * piece, piece)
        return pltpu.make_async_copy(
            feat_hbm.at[at, :, pl.ds(0, lanes)], xb.at[0, at], feat_sem.at[i]
        )

    def late_copy():
        return pltpu.make_async_copy(
            feat_hbm.at[:, :, pl.ds(lanes, lanes)], xb.at[1], late_sem
        )

    tables = [
        pltpu.make_async_copy(src, dst, index_sem.at[i])
        for i, (src, dst) in enumerate(
            (
                (srows_hbm, srows),
                (scnt_hbm, scnt),
                (lidx_hbm, lidx),
                (lcnt_hbm, lcnt),
                (hidx_hbm, hidx),
                (hcnt_hbm, hcnt),
            )
        )
    ]

    def w_load():
        mine = pl.ds(pl.multiple_of(d * shard, shard), shard)
        return pltpu.make_async_copy(weight_hbm.at[mine], wfull.at[z, d], wl_sem)

    for copy in tables[:2]:
        copy.start()
    for i in range(pieces):
        feat_copy(i).start()
    w_load().start()
    late_copy().start()
    for copy in tables[2:]:
        copy.start()

    barrier = pltpu.get_barrier_semaphore()
    for o in range(1, n_dom):
        pl.semaphore_signal(barrier, inc=1, device_id=(lax.rem(d + o, n_dom), z), device_id_type=MESH)
    for o in range(1, n_col):
        pl.semaphore_signal(barrier, inc=1, device_id=(d, lax.rem(z + o, n_col)), device_id_type=MESH)
    bfull[z] = jnp.broadcast_to(bias_ref[...].reshape(1, width), bfull.shape[1:])

    def widen(c, t):
        xf[c, pl.ds(pl.multiple_of(t * TILE, TILE), TILE), :] = xb[c, t].astype(jnp.float32)

    @pl.loop(0, pieces)
    def _(i):
        feat_copy(i).wait()
        for j in range(piece):
            widen(0, i * piece + j)

    def widen_late():
        late_copy().wait()

        @pl.loop(0, pieces)
        def _(i):
            for j in range(piece):
                widen(1, i * piece + j)

    def peer_of(i):
        side = i // n_chips
        at_mate = (i + 1) // n_chips - side
        over = 2 * lax.rem(chip + lax.rem(i, n_chips) + 1, n_chips) + side
        return over + at_mate * (1 - core)

    def slots_of(k, q):
        count = outs[k].shape[1]
        return pl.ds(q * count, count)

    def halo_send(k, peer):
        return remote(
            outs[k].at[peer], lands[k].at[slots_of(k, d)], halo_s.at[k], halo_r.at[k], (peer, z)
        )

    def halo_all(k):
        most = outs[k].at[pl.ds(0, n_dom - 1)]
        return remote(most, most, halo_s.at[k], halo_r.at[k], (mate, z))

    def first_lanes(shape):
        return lax.broadcasted_iota(jnp.int32, shape, len(shape) - 1) < lanes // 2

    def swap(x):
        return pltpu.roll(x, lanes // 2, x.ndim - 1)

    def fold(low, high):
        first, turned = first_lanes(low.shape), swap(high)
        return jnp.where(first, low, turned), jnp.where(first, turned, low)

    def unfold(a, b):
        first = first_lanes(a.shape)
        return jnp.where(first, a, b), swap(jnp.where(first, b, a))

    def picked_rows(c, peer):
        @pl.loop(0, slot_total // LANES)
        def _(g):
            group = pl.ds(pl.multiple_of(g * LANES, LANES), LANES)
            picked = srows.at[:, group]
            into = stage.at[group]
            for k in range(LANES):
                into[k] = xf[c, picked[peer, k]]

        used = lax.broadcasted_iota(jnp.int32, (slot_total, lanes), 0) < scnt[0, peer]
        return jnp.where(used, stage[...], 0.0)

    def gather_early(peer):
        sent = picked_rows(0, peer)
        a, b = fold(sent[: slot_total // 2], sent[slot_total // 2 :])
        out_a[peer] = a.astype(out_a.dtype).reshape(half_peer, TILE, lanes)
        out_b[peer] = b.astype(out_b.dtype).reshape(half_peer, TILE, lanes)

    def gather_late():
        @pl.loop(0, n_dom - 1)
        def _(i):
            peer = peer_of(i)
            sent = picked_rows(1, peer)
            out_late[peer] = sent.astype(out_late.dtype).reshape(per_peer, TILE, lanes)
            halo_send(2, peer).start()

    for copy in tables[:2]:
        copy.wait()
    gather_early(peer_of(0))
    lv_copy = pltpu.make_async_copy(lvals_hbm, lvals, vals_sem.at[0])
    hv_copy = pltpu.make_async_copy(hvals_hbm, hvals, vals_sem.at[1])
    lv_copy.start()
    hv_copy.start()
    pl.semaphore_wait(barrier, n_dom - 1 + n_col - 1)
    halo_send(0, peer_of(0)).start()

    @pl.loop(1, n_chips - 1)
    def _(i):
        gather_early(peer_of(i))
        halo_send(0, peer_of(i)).start()

    @pl.loop(0, n_chips - 1)
    def _(i):
        halo_send(1, peer_of(i)).start()

    def w_copy(o):
        return remote(wfull.at[z, d], wfull.at[z, d], w_s, w_r, (d, lax.rem(z + o, n_col)))

    def w_copies():
        some = pl.ds(0, n_col - 1)
        return remote(wfull.at[some, d], wfull.at[some, d], w_s, w_r, (d, lax.rem(z + 1, n_col)))

    def w_pass(o):
        return remote(wfull.at[:, d], wfull.at[:, d], wp_s, wp_r, (lax.rem(d + o, n_dom), z))

    def w_passes():
        most = pl.ds(0, n_dom - 1)
        return remote(wfull.at[:, most], wfull.at[:, most], wp_s, wp_r, (mate, z))

    def b_copy(o):
        return remote(bfull.at[z], bfull.at[z], b_s, b_r, (d, lax.rem(z + o, n_col)))

    def b_copies():
        some = bfull.at[pl.ds(0, n_col - 1)]
        return remote(some, some, b_s, b_r, (d, lax.rem(z + 1, n_col)))

    w_load().wait()
    for o in range(1, n_col):
        w_copy(o).start()
        b_copy(o).start()

    @pl.loop(n_chips - 1, n_dom - 1)
    def _(i):
        gather_early(peer_of(i))
        halo_send(0, peer_of(i)).start()
        halo_send(1, peer_of(i)).start()

    widen_late()
    for k in range(3):
        mine = slots_of(k, d)
        lands[k][mine] = jnp.zeros((outs[k].shape[1], TILE, lanes), halo_late.dtype)

    @pl.when(core == 1)
    def _():
        gather_late()

    for copy in tables[2:]:
        copy.wait()
    lv_copy.wait()
    hv_copy.wait()

    def kept(count, k):
        one = jnp.minimum(jnp.maximum(count - k, 0), 1).astype(jnp.float32)
        return jnp.broadcast_to(one, (TILE, TILE)).astype(jnp.bfloat16)

    def tile_rows(c, t):
        lhs, rhs = [], []
        n_loc, n_hal = lcnt[0, t], hcnt[0, t]
        for k in range(k_local):
            lhs.append(lvals[t, k] * kept(n_loc, k))
            rhs.append(xb[c, lidx[k, t]])
        for k in range(k_halo):
            lhs.append(hvals[t, k] * kept(n_hal, k))
            rhs.append(halos[c][hidx[k, t]])
        return jnp.dot(
            jnp.concatenate(lhs, axis=1),
            jnp.concatenate(rhs, axis=0),
            preferred_element_type=jnp.float32,
        )

    def p1_copy(c, s, o):
        return remote(
            tx.at[s, o - 1, c], rx.at[s, z, c], p1_s, p1_r.at[s], (d, lax.rem(z + o, n_col))
        )

    def p1_step(s):
        whole = tx.at[s]
        return remote(whole, whole, p1_s, p1_r.at[s], (d, lax.rem(z + 1, n_col)))

    def p1_part(s, o, k):
        at = pl.ds(k * (r_chunk // 2), r_chunk // 2)
        return remote(
            tx.at[s, o - 1, 0, at],
            rx.at[s, z, 0, at],
            p1_s,
            p1_r.at[s],
            (d, lax.rem(z + o, n_col)),
        )

    def folded(s, q, k):
        tiles = [tile_rows(0, q * tiles_q + s * ct + i) for i in range(ct)]
        pairs = [fold(tiles[i], tiles[i + ct // 2])[k] for i in range(ct // 2)]
        return jnp.concatenate(pairs, axis=0).astype(jnp.bfloat16)

    def early_step(s, k):
        at = pl.ds(k * (r_chunk // 2), r_chunk // 2)
        for o in range(1, n_col):
            tx[s, o - 1, 0, at, :] = folded(s, lax.rem(z + o, n_col), k)
            p1_part(s, o, k).start()

    def own_step(s):
        for k in range(2):
            at = pl.ds(k * (r_chunk // 2), r_chunk // 2)
            rx[s, z, 0, at, :] = folded(s, z, k)

    def full_step(c, s):
        for o in range(1, n_col):
            q = lax.rem(z + o, n_col)
            for i in range(ct):
                rows_i = tile_rows(c, q * tiles_q + s * ct + i)
                tx[s, o - 1, c, i * TILE : (i + 1) * TILE, :] = rows_i.astype(jnp.bfloat16)
            p1_copy(c, s, o).start()
        for i in range(ct):
            rows_i = tile_rows(c, z * tiles_q + s * ct + i)
            rx[s, z, c, i * TILE : (i + 1) * TILE, :] = rows_i.astype(jnp.bfloat16)

    def halves_of(land, q):
        return land[slots_of(0, q)].astype(jnp.float32)

    def place(q, k, tiles):
        at = pl.ds(q * per_peer + k * half_peer, half_peer)
        halo_early[at] = tiles.astype(halo_early.dtype)

    halo_all(0).wait_recv()

    @pl.loop(0, n_dom)
    def _(q):
        a = halves_of(land_a, q)
        place(q, 0, a)
        place(q, 1, swap(a))

    @pl.loop(0, EARLY_STEPS)
    def _(s):
        early_step(s, 0)

    halo_all(1).wait_recv()

    @pl.loop(0, n_dom)
    def _(q):
        low, high = unfold(halves_of(land_a, q), halves_of(land_b, q))
        place(q, 0, low)
        place(q, 1, high)

    @pl.loop(0, EARLY_STEPS)
    def _(s):
        early_step(s, 1)

    @pl.loop(EARLY_STEPS, steps)
    def _(s):
        full_step(0, s)

    @pl.loop(0, EARLY_STEPS)
    def _(s):
        own_step(s)

    @pl.when(core == 0)
    def _():
        gather_late()

    w_copies().wait_recv()

    @pl.loop(1, n_dom)
    def _(o):
        w_pass(o).start()

    halo_all(2).wait_recv()

    @pl.loop(0, steps)
    def _(s):
        full_step(1, s)

    w_passes().wait_recv()
    b_copies().wait()

    acc[...] = jnp.zeros_like(acc)

    def out_rows(s):
        return pl.ds(pl.multiple_of(z * rows_q + s * r_out, r_out), r_out)

    def p2_copy(s, o):
        q = lax.rem(z + o, n_col)
        return remote(tx2.at[s, q], out_hbm.at[out_rows(s)], p2_s, p2_r, (d, q))

    def p2_all():
        most = tx2.at[:, pl.ds(0, n_col - 1)]
        return remote(most, most, p2_s, p2_r, (d, lax.rem(z + 1, n_col)))

    def own_copy(s):
        return pltpu.make_async_copy(tx2.at[s, z], out_hbm.at[out_rows(s)], own_sem)

    def own_all():
        mine = tx2.at[:, z]
        return pltpu.make_async_copy(mine, mine, own_sem)

    @pl.loop(0, steps)
    def _(s):
        p1_step(s).wait_recv()

        @pl.when(s < EARLY_STEPS)
        def _():
            for j in range(n_col):
                a = rx[s, j, 0, : r_chunk // 2, :].astype(jnp.float32)
                b = rx[s, j, 0, r_chunk // 2 :, :].astype(jnp.float32)
                low, high = unfold(a, b)
                rx[s, j, 0, : r_chunk // 2, :] = low.astype(jnp.bfloat16)
                rx[s, j, 0, r_chunk // 2 :, :] = high.astype(jnp.bfloat16)

        @pl.loop(0, halves)
        def _(h):
            k = s * halves + h
            at = pl.ds(pl.multiple_of(h * r_out, r_out), r_out)
            mixed = jnp.concatenate(
                [rx[s, j, c, at, :] for j in range(n_col) for c in range(n_part)], axis=1
            )
            power = jnp.zeros((r_out, 1), jnp.float32)
            active = []
            for j in range(n_col):
                y = jnp.dot(
                    mixed, wfull[j].reshape(f_total, width), preferred_element_type=jnp.float32
                )
                y = jnp.maximum(y + bfull[j][0:1, :].astype(jnp.float32), 0.0)
                power = power + jnp.sum(y * y, axis=1, keepdims=True)
                active.append(y)
            factor = lax.rsqrt(power / f_total + epsilon)
            for j in range(n_col):
                scaled = active[j] * factor
                tx2[k, j] = scaled.astype(jnp.bfloat16)
                grouped = scaled.reshape(r_out // 8, 8, width)
                acc[j, 0] += jnp.sum(grouped, axis=0)
                acc[j, 1] += jnp.sum(grouped * grouped, axis=0)
            for o in range(1, n_col):
                p2_copy(k, o).start()
            own_copy(k).start()

    for j in range(n_col):
        part[j] = jnp.concatenate(
            [
                jnp.sum(acc[j, 0], axis=0, keepdims=True),
                jnp.sum(acc[j, 1], axis=0, keepdims=True),
                jnp.zeros((6, width), jnp.float32),
            ],
            axis=0,
        )

    def sd_copy(o):
        return remote(part, part_in.at[o], sd_s, sd_r, (lax.rem(d + o, n_dom), z))

    def sd_all():
        most = part_in.at[pl.ds(1, n_dom - 1)]
        return remote(most, most, sd_s, sd_r, (mate, z))

    @pl.loop(1, n_dom)
    def _(o):
        sd_copy(o).start()

    part_in[0] = part[...]
    sd_all().wait()
    colpart[...] = jnp.sum(part_in[...], axis=0)

    def sc_copy(o):
        q = lax.rem(z + o, n_col)
        return remote(colpart.at[q], colpart_in.at[o], sc_s, sc_r, (d, q))

    def sc_all():
        some = colpart_in.at[pl.ds(1, n_col - 1)]
        return remote(some, some, sc_s, sc_r, (d, lax.rem(z + 1, n_col)))

    for o in range(1, n_col):
        sc_copy(o).start()
    colpart_in[0] = colpart[z]

    w_copies().wait_send()
    w_passes().wait_send()
    for k in range(3):
        halo_all(k).wait_send()

    remote(tx, tx, p1_s, p1_r.at[0], (d, lax.rem(z + 1, n_col))).wait_send()
    sc_all().wait()
    totals = jnp.sum(colpart_in[...], axis=0) / node_total
    mean = totals[0:1, :]
    stat_ref[...] = jnp.concatenate([mean, totals[1:2, :] - mean * mean], axis=0)

    p2_all().wait()
    own_all().wait()


def on_device(
    features,
    weight,
    out_bias,
    local_index,
    local_count,
    local_vals,
    halo_index,
    halo_count,
    halo_vals,
    send_rows,
    send_count,
):
    rows, width = features.shape
    n_dom = lax.axis_size("dom")
    n_col = lax.axis_size("col")
    slot_total = send_rows.shape[2]
    f_total = weight.shape[0]
    n_part = width // LANES
    steps = rows // TILE // n_col // P1_TILES
    steps_out = rows // TILE // n_col // P2_TILES
    r_chunk = P1_TILES * TILE
    r_out = P2_TILES * TILE
    pieces = 8 if rows // TILE % 8 == 0 else 1
    any_spec = pl.BlockSpec(memory_space=pl.ANY)
    vmem = pl.BlockSpec(memory_space=pltpu.VMEM)
    bf16, f32 = jnp.bfloat16, jnp.float32
    dma = pltpu.SemaphoreType.DMA

    def table(*shape):
        return pltpu.SMEM(shape, jnp.int32)

    halo_bytes = 4 * n_dom * slot_total * width
    grant = 44 * 2**20 + 2 * halo_bytes
    held = pltpu.VMEM if grant + 2 * rows * width < 58 * 2**20 else jax.ShapeDtypeStruct
    grant = grant if held is pltpu.VMEM else 67043328
    normalized, stats = pl.pallas_call(
        functools.partial(kernel, n_dom, n_col, rows * n_dom),
        out_shape=(
            held((rows, width), bf16),
            held((2, width), f32),
        ),
        in_specs=[any_spec, any_spec, vmem] + [any_spec] * 8,
        out_specs=(any_spec, vmem),
        scratch_shapes=[
            pltpu.VMEM((n_part, rows // TILE, TILE, LANES), bf16),
            pltpu.VMEM((n_part, rows, LANES), f32),
            pltpu.VMEM((slot_total, LANES), f32),
            pltpu.VMEM((n_dom, slot_total // TILE // 2, TILE, LANES), bf16),
            pltpu.VMEM((n_dom, slot_total // TILE // 2, TILE, LANES), bf16),
            pltpu.VMEM((n_dom, slot_total // TILE, TILE, LANES), bf16),
            pltpu.VMEM((n_dom * slot_total // TILE // 2, TILE, LANES), bf16),
            pltpu.VMEM((n_dom * slot_total // TILE // 2, TILE, LANES), bf16),
            pltpu.VMEM((n_dom * slot_total // TILE, TILE, LANES), bf16),
            pltpu.VMEM((n_dom * slot_total // TILE, TILE, LANES), bf16),
            pltpu.VMEM(local_vals.shape[1:], bf16),
            pltpu.VMEM(halo_vals.shape[1:], bf16),
            pltpu.VMEM((n_col, n_dom, f_total // n_dom, width), bf16),
            pltpu.VMEM((n_col, 16, width), bf16),
            pltpu.VMEM((steps, n_col - 1, n_part, r_chunk, LANES), bf16),
            pltpu.VMEM((steps, n_col, n_part, r_chunk, LANES), bf16),
            pltpu.VMEM((steps_out, n_col, r_out, width), bf16),
            pltpu.VMEM((n_col, 2, 8, width), f32),
            pltpu.VMEM((n_col, 8, width), f32),
            pltpu.VMEM((n_dom, n_col, 8, width), f32),
            pltpu.VMEM((n_col, 8, width), f32),
            pltpu.VMEM((n_col, 8, width), f32),
            table(local_index.shape[2], rows // TILE),
            table(1, rows // TILE),
            table(halo_index.shape[2], rows // TILE),
            table(1, rows // TILE),
            table(n_dom, slot_total),
            table(1, n_dom),
            dma((pieces,)),
            dma,
            dma((6,)),
            dma((2,)),
            dma,
            dma((3,)),
            dma((3,)),
            dma,
            dma,
            dma,
            dma,
            dma,
            dma,
            dma,
            dma((steps,)),
            dma,
            dma,
            dma,
            dma,
            dma,
            dma,
            dma,
        ],
        compiler_params=pltpu.CompilerParams(
            collective_id=0, has_side_effects=True, vmem_limit_bytes=grant
        ),
    )(
        features.reshape(rows // TILE, TILE, width),
        weight,
        out_bias,
        local_index[0].T,
        local_count,
        local_vals[0],
        halo_index[0].T,
        halo_count,
        halo_vals[0],
        send_rows[0],
        send_count,
    )
    return normalized, stats


def solution(mesh):
    in_specs = (
        P("dom", "col"),
        P(None, "col"),
        P("col"),
        P("dom", None, None),
        P("dom", None),
        P("dom", None, None, None, None),
        P("dom", None, None),
        P("dom", None),
        P("dom", None, None, None, None),
        P("dom", None, None),
        P("dom", None),
    )
    out_specs = (P("dom", "col"), P(None, "col"))
    return jax.shard_map(
        on_device, mesh=mesh, in_specs=in_specs, out_specs=out_specs, check_vma=False
    )
```

```python
import functools

import jax
import jax.numpy as jnp
from jax import lax
from jax.experimental import pallas as pl
from jax.experimental.pallas import tpu as pltpu
from jax.sharding import PartitionSpec as P

TILE = 128
MESH = pl.DeviceIdType.MESH
LANES = 128
P1_TILES = 4
P2_TILES = 2
EARLY_STEPS = 1
epsilon = 1e-06


def remote(src, dst, send_sem, recv_sem, device):
    return pltpu.make_async_remote_copy(
        src_ref=src,
        dst_ref=dst,
        send_sem=send_sem,
        recv_sem=recv_sem,
        device_id=device,
        device_id_type=MESH,
    )


def kernel(
    n_dom,
    n_col,
    node_total,
    feat_hbm,
    weight_hbm,
    bias_ref,
    lidx_hbm,
    lcnt_hbm,
    lvals_hbm,
    hidx_hbm,
    hcnt_hbm,
    hvals_hbm,
    srows_hbm,
    scnt_hbm,
    out_hbm,
    stat_ref,
    xb_early,
    xb_late,
    xf,
    stage,
    out_a,
    out_b,
    out_late,
    land_a,
    land_b,
    halo_early,
    halo_late,
    lvals,
    hvals,
    wfull,
    bfull,
    tx,
    rx,
    tx2,
    acc,
    part,
    part_in,
    colpart,
    colpart_in,
    lidx,
    lcnt,
    hidx,
    hcnt,
    srows,
    scnt,
    feat_sem,
    late_sem,
    index_sem,
    vals_sem,
    wl_sem,
    halo_s,
    halo_r,
    w_s,
    w_r,
    wp_s,
    wp_r,
    b_s,
    b_r,
    p1_s,
    p1_r,
    p2_s,
    p2_r,
    own_sem,
    sd_s,
    sd_r,
    sc_s,
    sc_r,
):
    d = lax.axis_index("dom")
    z = lax.axis_index("col")
    halos = (halo_early, halo_late)
    xb = (xb_early, xb_late)
    outs = (out_a, out_b, out_late)
    lands = (land_a, land_b, halo_late)
    n_part, rows, lanes = xf.shape
    width = n_part * lanes
    slot_total = srows_hbm.shape[1]
    k_local = lvals.shape[1]
    k_halo = hvals.shape[1]
    f_total = weight_hbm.shape[0]
    tiles_q = rows // TILE // n_col
    rows_q = tiles_q * TILE
    ct = P1_TILES
    r_chunk = ct * TILE
    steps = tiles_q // ct
    r_out = P2_TILES * TILE
    halves = r_chunk // r_out
    per_peer = slot_total // TILE
    half_peer = per_peer // 2
    shard = f_total // n_dom
    n_chips = n_dom // 2
    chip = d // 2
    core = lax.rem(d, 2)
    mate = d + 1 - 2 * core

    pieces = feat_sem.shape[0]
    piece = rows // TILE // pieces

    def feat_copy(i):
        at = pl.ds(i * piece, piece)
        return pltpu.make_async_copy(
            feat_hbm.at[at, :, pl.ds(0, lanes)], xb_early.at[at], feat_sem.at[i]
        )

    def late_copy():
        return pltpu.make_async_copy(
            feat_hbm.at[:, :, pl.ds(lanes, lanes)], xb_late, late_sem
        )

    groups = srows.shape[0]
    pairs = [(srows_hbm.at[:, pl.ds(g * LANES, LANES)], srows.at[g]) for g in range(groups)]
    pairs += [(scnt_hbm, scnt), (lidx_hbm, lidx), (lcnt_hbm, lcnt), (hidx_hbm, hidx), (hcnt_hbm, hcnt)]
    tables = [
        pltpu.make_async_copy(src, dst, index_sem.at[i]) for i, (src, dst) in enumerate(pairs)
    ]
    first_tables, other_tables = tables[: groups + 1], tables[groups + 1 :]

    def w_load():
        mine = pl.ds(pl.multiple_of(d * shard, shard), shard)
        return pltpu.make_async_copy(weight_hbm.at[mine], wfull.at[z, d], wl_sem)

    for copy in first_tables:
        copy.start()
    for i in range(pieces):
        feat_copy(i).start()
    w_load().start()
    for copy in other_tables:
        copy.start()
    lv_copy = pltpu.make_async_copy(lvals_hbm, lvals, vals_sem.at[0])
    hv_copy = pltpu.make_async_copy(hvals_hbm, hvals, vals_sem.at[1])

    barrier = pltpu.get_barrier_semaphore()
    for o in range(1, n_dom):
        pl.semaphore_signal(barrier, inc=1, device_id=(lax.rem(d + o, n_dom), z), device_id_type=MESH)
    for o in range(1, n_col):
        pl.semaphore_signal(barrier, inc=1, device_id=(d, lax.rem(z + o, n_col)), device_id_type=MESH)
    bfull[z] = jnp.broadcast_to(bias_ref[...].reshape(1, width), bfull.shape[1:])

    def slots_of(k, q):
        count = outs[k].shape[1]
        return pl.ds(q * count, count)

    for k in range(3):
        mine = slots_of(k, d)
        lands[k][mine] = jnp.zeros((outs[k].shape[1], TILE, lanes), halo_late.dtype)
    acc[...] = jnp.zeros_like(acc)

    def widen(c, t):
        xf[c, pl.ds(pl.multiple_of(t * TILE, TILE), TILE), :] = xb[c][t].astype(jnp.float32)

    @pl.loop(0, pieces)
    def _(i):
        feat_copy(i).wait()
        for j in range(piece):
            widen(0, i * piece + j)

    lv_copy.start()
    hv_copy.start()
    late_copy().start()

    def widen_late():
        late_copy().wait()

        @pl.loop(0, pieces)
        def _(i):
            for j in range(piece):
                widen(1, i * piece + j)

    def peer_of(i):
        side = i // n_chips
        at_mate = (i + 1) // n_chips - side
        over = 2 * lax.rem(chip + lax.rem(i, n_chips) + 1, n_chips) + side
        return over + at_mate * (1 - core)

    def halo_send(k, peer):
        return remote(
            outs[k].at[peer], lands[k].at[slots_of(k, d)], halo_s.at[k], halo_r.at[k], (peer, z)
        )

    def halo_all(k):
        most = outs[k].at[pl.ds(0, n_dom - 1)]
        return remote(most, most, halo_s.at[k], halo_r.at[k], (mate, z))

    def first_lanes(shape):
        return lax.broadcasted_iota(jnp.int32, shape, len(shape) - 1) < lanes // 2

    def swap(x):
        return pltpu.roll(x, lanes // 2, x.ndim - 1)

    def fold(low, high):
        first, turned = first_lanes(low.shape), swap(high)
        return jnp.where(first, low, turned), jnp.where(first, turned, low)

    def unfold(a, b):
        first = first_lanes(a.shape)
        return jnp.where(first, a, b), swap(jnp.where(first, b, a))

    def picked_rows(c, peer):
        @pl.loop(0, slot_total // LANES)
        def _(g):
            group = pl.ds(pl.multiple_of(g * LANES, LANES), LANES)
            into = stage.at[group]
            for k in range(LANES):
                into[k] = xf[c, srows[g, peer, k]]

        used = lax.broadcasted_iota(jnp.int32, (slot_total, lanes), 0) < scnt[0, peer]
        return jnp.where(used, stage[...], 0.0)

    def gather_early(peer):
        sent = picked_rows(0, peer)
        a, b = fold(sent[: slot_total // 2], sent[slot_total // 2 :])
        out_a[peer] = a.astype(out_a.dtype).reshape(half_peer, TILE, lanes)
        out_b[peer] = b.astype(out_b.dtype).reshape(half_peer, TILE, lanes)

    def gather_late():
        @pl.loop(0, n_dom - 1)
        def _(i):
            peer = peer_of(i)
            sent = picked_rows(1, peer)
            out_late[peer] = sent.astype(out_late.dtype).reshape(per_peer, TILE, lanes)
            halo_send(2, peer).start()

    for copy in first_tables:
        copy.wait()
    gather_early(peer_of(0))
    pl.semaphore_wait(barrier, n_dom - 1 + n_col - 1)
    halo_send(0, peer_of(0)).start()

    @pl.loop(1, n_chips - 1)
    def _(i):
        gather_early(peer_of(i))
        halo_send(0, peer_of(i)).start()

    @pl.loop(0, n_chips - 1)
    def _(i):
        halo_send(1, peer_of(i)).start()

    def w_copy(o):
        return remote(wfull.at[z, d], wfull.at[z, d], w_s, w_r, (d, lax.rem(z + o, n_col)))

    def w_copies():
        some = pl.ds(0, n_col - 1)
        return remote(wfull.at[some, d], wfull.at[some, d], w_s, w_r, (d, lax.rem(z + 1, n_col)))

    def w_pass(o):
        return remote(wfull.at[:, d], wfull.at[:, d], wp_s, wp_r, (lax.rem(d + o, n_dom), z))

    def w_passes():
        most = pl.ds(0, n_dom - 1)
        return remote(wfull.at[:, most], wfull.at[:, most], wp_s, wp_r, (mate, z))

    def b_copy(o):
        return remote(bfull.at[z], bfull.at[z], b_s, b_r, (d, lax.rem(z + o, n_col)))

    def b_copies():
        some = bfull.at[pl.ds(0, n_col - 1)]
        return remote(some, some, b_s, b_r, (d, lax.rem(z + 1, n_col)))

    w_load().wait()
    for o in range(1, n_col):
        w_copy(o).start()
        b_copy(o).start()

    @pl.loop(n_chips - 1, n_dom - 1)
    def _(i):
        gather_early(peer_of(i))
        halo_send(0, peer_of(i)).start()
        halo_send(1, peer_of(i)).start()

    @pl.when(core == 1)
    def _():
        widen_late()
        gather_late()

    for copy in other_tables:
        copy.wait()
    lv_copy.wait()
    hv_copy.wait()

    def kept(count, k):
        one = jnp.minimum(jnp.maximum(count - k, 0), 1).astype(jnp.float32)
        return jnp.broadcast_to(one, (TILE, TILE)).astype(jnp.bfloat16)

    def tile_rows(c, t):
        lhs, rhs = [], []
        n_loc, n_hal = lcnt[0, t], hcnt[0, t]
        for k in range(k_local):
            lhs.append(lvals[t, k] * kept(n_loc, k))
            rhs.append(xb[c][lidx[k, t]])
        for k in range(k_halo):
            lhs.append(hvals[t, k] * kept(n_hal, k))
            rhs.append(halos[c][hidx[k, t]])
        return jnp.dot(
            jnp.concatenate(lhs, axis=1),
            jnp.concatenate(rhs, axis=0),
            preferred_element_type=jnp.float32,
        )

    def p1_copy(c, s, o):
        return remote(
            tx.at[s, o - 1, c], rx.at[s, z, c], p1_s, p1_r.at[s], (d, lax.rem(z + o, n_col))
        )

    def p1_step(s):
        whole = tx.at[s]
        return remote(whole, whole, p1_s, p1_r.at[s], (d, lax.rem(z + 1, n_col)))

    def p1_part(s, o, k):
        at = pl.ds(k * (r_chunk // 2), r_chunk // 2)
        return remote(
            tx.at[s, o - 1, 0, at],
            rx.at[s, z, 0, at],
            p1_s,
            p1_r.at[s],
            (d, lax.rem(z + o, n_col)),
        )

    def folded(s, q, k):
        tiles = [tile_rows(0, q * tiles_q + s * ct + i) for i in range(ct)]
        pairs = [fold(tiles[i], tiles[i + ct // 2])[k] for i in range(ct // 2)]
        return jnp.concatenate(pairs, axis=0).astype(jnp.bfloat16)

    def early_step(s, k):
        at = pl.ds(k * (r_chunk // 2), r_chunk // 2)
        for o in range(1, n_col):
            tx[s, o - 1, 0, at, :] = folded(s, lax.rem(z + o, n_col), k)
            p1_part(s, o, k).start()

    def own_step(s):
        for k in range(2):
            at = pl.ds(k * (r_chunk // 2), r_chunk // 2)
            rx[s, z, 0, at, :] = folded(s, z, k)

    def full_step(c, s):
        for o in range(1, n_col):
            q = lax.rem(z + o, n_col)
            for i in range(ct):
                rows_i = tile_rows(c, q * tiles_q + s * ct + i)
                tx[s, o - 1, c, i * TILE : (i + 1) * TILE, :] = rows_i.astype(jnp.bfloat16)
            p1_copy(c, s, o).start()
        for i in range(ct):
            rows_i = tile_rows(c, z * tiles_q + s * ct + i)
            rx[s, z, c, i * TILE : (i + 1) * TILE, :] = rows_i.astype(jnp.bfloat16)

    def halves_of(land, q):
        return land[slots_of(0, q)].astype(jnp.float32)

    def place(q, k, tiles):
        at = pl.ds(q * per_peer + k * half_peer, half_peer)
        halo_early[at] = tiles.astype(halo_early.dtype)

    halo_all(0).wait_recv()

    @pl.loop(0, n_dom)
    def _(q):
        a = halves_of(land_a, q)
        place(q, 0, a)
        place(q, 1, swap(a))

    @pl.loop(0, EARLY_STEPS)
    def _(s):
        early_step(s, 0)

    halo_all(1).wait_recv()

    @pl.loop(0, n_dom)
    def _(q):
        low, high = unfold(halves_of(land_a, q), halves_of(land_b, q))
        place(q, 0, low)
        place(q, 1, high)

    @pl.loop(0, EARLY_STEPS)
    def _(s):
        early_step(s, 1)

    @pl.loop(EARLY_STEPS, steps)
    def _(s):
        full_step(0, s)

    @pl.loop(0, EARLY_STEPS)
    def _(s):
        own_step(s)

    @pl.when(core == 0)
    def _():
        widen_late()
        gather_late()

    w_copies().wait_recv()

    @pl.loop(1, n_dom)
    def _(o):
        w_pass(o).start()

    halo_all(2).wait_recv()

    @pl.loop(0, steps)
    def _(s):
        full_step(1, s)

    w_passes().wait_recv()
    b_copies().wait()

    def out_rows(s):
        return pl.ds(pl.multiple_of(z * rows_q + s * r_out, r_out), r_out)

    def p2_copy(s, o):
        q = lax.rem(z + o, n_col)
        return remote(tx2.at[s, q], out_hbm.at[out_rows(s)], p2_s, p2_r, (d, q))

    def p2_all():
        most = tx2.at[:, pl.ds(0, n_col - 1)]
        return remote(most, most, p2_s, p2_r, (d, lax.rem(z + 1, n_col)))

    def own_copy(s):
        return pltpu.make_async_copy(tx2.at[s, z], out_hbm.at[out_rows(s)], own_sem)

    def own_all():
        mine = tx2.at[:, z]
        return pltpu.make_async_copy(mine, mine, own_sem)

    @pl.loop(0, steps)
    def _(s):
        p1_step(s).wait_recv()

        @pl.when(s < EARLY_STEPS)
        def _():
            for j in range(n_col):
                a = rx[s, j, 0, : r_chunk // 2, :].astype(jnp.float32)
                b = rx[s, j, 0, r_chunk // 2 :, :].astype(jnp.float32)
                low, high = unfold(a, b)
                rx[s, j, 0, : r_chunk // 2, :] = low.astype(jnp.bfloat16)
                rx[s, j, 0, r_chunk // 2 :, :] = high.astype(jnp.bfloat16)

        @pl.loop(0, halves)
        def _(h):
            k = s * halves + h
            at = pl.ds(pl.multiple_of(h * r_out, r_out), r_out)
            mixed = jnp.concatenate(
                [rx[s, j, c, at, :] for j in range(n_col) for c in range(n_part)], axis=1
            )
            power = jnp.zeros((r_out, 1), jnp.float32)
            active = []
            for j in range(n_col):
                y = jnp.dot(
                    mixed, wfull[j].reshape(f_total, width), preferred_element_type=jnp.float32
                )
                y = jnp.maximum(y + bfull[j][0:1, :].astype(jnp.float32), 0.0)
                power = power + jnp.sum(y * y, axis=1, keepdims=True)
                active.append(y)
            factor = lax.rsqrt(power / f_total + epsilon)
            for j in range(n_col):
                scaled = active[j] * factor
                tx2[k, j] = scaled.astype(jnp.bfloat16)
                grouped = scaled.reshape(r_out // 8, 8, width)
                acc[j, 0] += jnp.sum(grouped, axis=0)
                acc[j, 1] += jnp.sum(grouped * grouped, axis=0)
            for o in range(1, n_col):
                p2_copy(k, o).start()
            own_copy(k).start()

    for j in range(n_col):
        part[j] = jnp.concatenate(
            [
                jnp.sum(acc[j, 0], axis=0, keepdims=True),
                jnp.sum(acc[j, 1], axis=0, keepdims=True),
                jnp.zeros((6, width), jnp.float32),
            ],
            axis=0,
        )

    def sd_copy(o):
        return remote(part, part_in.at[o], sd_s, sd_r, (lax.rem(d + o, n_dom), z))

    def sd_all():
        most = part_in.at[pl.ds(1, n_dom - 1)]
        return remote(most, most, sd_s, sd_r, (mate, z))

    @pl.loop(1, n_dom)
    def _(o):
        sd_copy(o).start()

    part_in[0] = part[...]
    sd_all().wait()
    colpart[...] = jnp.sum(part_in[...], axis=0)

    def sc_copy(o):
        q = lax.rem(z + o, n_col)
        return remote(colpart.at[q], colpart_in.at[o], sc_s, sc_r, (d, q))

    def sc_all():
        some = colpart_in.at[pl.ds(1, n_col - 1)]
        return remote(some, some, sc_s, sc_r, (d, lax.rem(z + 1, n_col)))

    for o in range(1, n_col):
        sc_copy(o).start()
    colpart_in[0] = colpart[z]

    w_copies().wait_send()
    w_passes().wait_send()
    for k in range(3):
        halo_all(k).wait_send()

    remote(tx, tx, p1_s, p1_r.at[0], (d, lax.rem(z + 1, n_col))).wait_send()
    sc_all().wait()
    totals = jnp.sum(colpart_in[...], axis=0) / node_total
    mean = totals[0:1, :]
    stat_ref[...] = jnp.concatenate([mean, totals[1:2, :] - mean * mean], axis=0)

    p2_all().wait()
    own_all().wait()


def flush(rows_ref, stat_ref, out_hbm, stat_hbm, row_sem, stat_sem):
    small = pltpu.make_async_copy(stat_ref, stat_hbm, stat_sem)
    small.start()
    piece = out_hbm.shape[0] // 8
    for i in range(8):
        at = pl.ds(i * piece, piece)
        pltpu.make_async_copy(rows_ref.at[at], out_hbm.at[at], row_sem).start()
    pltpu.make_async_copy(rows_ref, out_hbm, row_sem).wait()
    small.wait()


def on_device(
    features,
    weight,
    out_bias,
    local_index,
    local_count,
    local_vals,
    halo_index,
    halo_count,
    halo_vals,
    send_rows,
    send_count,
):
    rows, width = features.shape
    n_dom = lax.axis_size("dom")
    n_col = lax.axis_size("col")
    slot_total = send_rows.shape[2]
    f_total = weight.shape[0]
    n_part = width // LANES
    steps = rows // TILE // n_col // P1_TILES
    steps_out = rows // TILE // n_col // P2_TILES
    r_chunk = P1_TILES * TILE
    r_out = P2_TILES * TILE
    pieces = 8 if rows // TILE % 8 == 0 else 1
    any_spec = pl.BlockSpec(memory_space=pl.ANY)
    vmem = pl.BlockSpec(memory_space=pltpu.VMEM)
    bf16, f32 = jnp.bfloat16, jnp.float32
    dma = pltpu.SemaphoreType.DMA

    def table(*shape):
        return pltpu.SMEM(shape, jnp.int32)

    halo_bytes = 4 * n_dom * slot_total * width
    grant = 44 * 2**20 + 2 * halo_bytes
    held = pltpu.VMEM if grant + 2 * rows * width < 58 * 2**20 else jax.ShapeDtypeStruct
    grant = grant if held is pltpu.VMEM else 67043328
    normalized, stats = pl.pallas_call(
        functools.partial(kernel, n_dom, n_col, rows * n_dom),
        out_shape=(
            held((rows, width), bf16),
            held((2, width), f32),
        ),
        in_specs=[any_spec, any_spec, vmem] + [any_spec] * 8,
        out_specs=(any_spec, vmem),
        scratch_shapes=[
            pltpu.VMEM((rows // TILE, TILE, LANES), bf16),
            pltpu.VMEM((rows // TILE, TILE, LANES), bf16),
            pltpu.VMEM((n_part, rows, LANES), f32),
            pltpu.VMEM((slot_total, LANES), f32),
            pltpu.VMEM((n_dom, slot_total // TILE // 2, TILE, LANES), bf16),
            pltpu.VMEM((n_dom, slot_total // TILE // 2, TILE, LANES), bf16),
            pltpu.VMEM((n_dom, slot_total // TILE, TILE, LANES), bf16),
            pltpu.VMEM((n_dom * slot_total // TILE // 2, TILE, LANES), bf16),
            pltpu.VMEM((n_dom * slot_total // TILE // 2, TILE, LANES), bf16),
            pltpu.VMEM((n_dom * slot_total // TILE, TILE, LANES), bf16),
            pltpu.VMEM((n_dom * slot_total // TILE, TILE, LANES), bf16),
            pltpu.VMEM(local_vals.shape[1:], bf16),
            pltpu.VMEM(halo_vals.shape[1:], bf16),
            pltpu.VMEM((n_col, n_dom, f_total // n_dom, width), bf16),
            pltpu.VMEM((n_col, 16, width), bf16),
            pltpu.VMEM((steps, n_col - 1, n_part, r_chunk, LANES), bf16),
            pltpu.VMEM((steps, n_col, n_part, r_chunk, LANES), bf16),
            pltpu.VMEM((steps_out, n_col, r_out, width), bf16),
            pltpu.VMEM((n_col, 2, 8, width), f32),
            pltpu.VMEM((n_col, 8, width), f32),
            pltpu.VMEM((n_dom, n_col, 8, width), f32),
            pltpu.VMEM((n_col, 8, width), f32),
            pltpu.VMEM((n_col, 8, width), f32),
            table(local_index.shape[2], rows // TILE),
            table(1, rows // TILE),
            table(halo_index.shape[2], rows // TILE),
            table(1, rows // TILE),
            table(slot_total // LANES, n_dom, LANES),
            table(1, n_dom),
            dma((pieces,)),
            dma,
            dma((slot_total // LANES + 5,)),
            dma((2,)),
            dma,
            dma((3,)),
            dma((3,)),
            dma,
            dma,
            dma,
            dma,
            dma,
            dma,
            dma,
            dma((steps,)),
            dma,
            dma,
            dma,
            dma,
            dma,
            dma,
            dma,
        ],
        compiler_params=pltpu.CompilerParams(
            collective_id=0, has_side_effects=True, vmem_limit_bytes=grant
        ),
    )(
        features.reshape(rows // TILE, TILE, width),
        weight,
        out_bias,
        local_index[0].T,
        local_count,
        local_vals[0],
        halo_index[0].T,
        halo_count,
        halo_vals[0],
        send_rows[0],
        send_count,
    )
    if held is not pltpu.VMEM:
        return normalized, stats
    return pl.pallas_call(
        flush,
        out_shape=(
            jax.ShapeDtypeStruct((rows, width), bf16),
            jax.ShapeDtypeStruct((2, width), f32),
        ),
        in_specs=[vmem, vmem],
        out_specs=(any_spec, any_spec),
        scratch_shapes=[dma, dma],
        compiler_params=pltpu.CompilerParams(vmem_limit_bytes=16 * 2**20),
    )(normalized, stats)


def solution(mesh):
    in_specs = (
        P("dom", "col"),
        P(None, "col"),
        P("col"),
        P("dom", None, None),
        P("dom", None),
        P("dom", None, None, None, None),
        P("dom", None, None),
        P("dom", None),
        P("dom", None, None, None, None),
        P("dom", None, None),
        P("dom", None),
    )
    out_specs = (P("dom", "col"), P(None, "col"))
    return jax.shard_map(
        on_device, mesh=mesh, in_specs=in_specs, out_specs=out_specs, check_vma=False
    )
```

```python
import functools

import jax
import jax.numpy as jnp
from jax import lax
from jax.experimental import pallas as pl
from jax.experimental.pallas import tpu as pltpu
from jax.sharding import PartitionSpec as P

TILE = 128
MESH = pl.DeviceIdType.MESH
LANES = 128
P1_TILES = 4
P2_TILES = 2
EARLY_STEPS = 1
epsilon = 1e-06


def remote(src, dst, send_sem, recv_sem, device):
    return pltpu.make_async_remote_copy(
        src_ref=src,
        dst_ref=dst,
        send_sem=send_sem,
        recv_sem=recv_sem,
        device_id=device,
        device_id_type=MESH,
    )


def kernel(
    n_dom,
    n_col,
    node_total,
    feat_hbm,
    weight_hbm,
    bias_ref,
    lidx_hbm,
    lcnt_hbm,
    lvals_hbm,
    hidx_hbm,
    hcnt_hbm,
    hvals_hbm,
    srows_hbm,
    scnt_hbm,
    out_hbm,
    stat_ref,
    xb_early,
    xb_late,
    xf,
    stage,
    out_a,
    out_b,
    out_late,
    land_a,
    land_b,
    halo_early,
    halo_late,
    lvals,
    hvals,
    wfull,
    bfull,
    tx,
    rx,
    tx2,
    acc,
    part,
    part_in,
    colpart,
    colpart_in,
    lidx,
    lcnt,
    hidx,
    hcnt,
    srows,
    scnt,
    feat_sem,
    late_sem,
    index_sem,
    vals_sem,
    wl_sem,
    halo_s,
    halo_r,
    w_s,
    w_r,
    wp_s,
    wp_r,
    b_s,
    b_r,
    p1_s,
    p1_r,
    p2_s,
    p2_r,
    own_sem,
    sd_s,
    sd_r,
    sc_s,
    sc_r,
):
    d = lax.axis_index("dom")
    z = lax.axis_index("col")
    halos = (halo_early, halo_late)
    xb = (xb_early, xb_late)
    outs = (out_a, out_b, out_late)
    lands = (land_a, land_b, halo_late)
    n_part, rows, lanes = xf.shape
    width = n_part * lanes
    slot_total = srows_hbm.shape[1]
    k_local = lvals.shape[1]
    k_halo = hvals.shape[1]
    f_total = weight_hbm.shape[0]
    tiles_q = rows // TILE // n_col
    rows_q = tiles_q * TILE
    ct = P1_TILES
    r_chunk = ct * TILE
    steps = tiles_q // ct
    r_out = P2_TILES * TILE
    halves = r_chunk // r_out
    per_peer = slot_total // TILE
    half_peer = per_peer // 2
    shard = f_total // n_dom
    n_chips = n_dom // 2
    chip = d // 2
    core = lax.rem(d, 2)
    mate = d + 1 - 2 * core

    pieces = feat_sem.shape[0]
    piece = rows // TILE // pieces

    def feat_copy(i):
        at = pl.ds(i * piece, piece)
        return pltpu.make_async_copy(
            feat_hbm.at[at, :, pl.ds(0, lanes)], xb_early.at[at], feat_sem.at[i]
        )

    def late_copy():
        return pltpu.make_async_copy(
            feat_hbm.at[:, :, pl.ds(lanes, lanes)], xb_late, late_sem
        )

    groups = srows.shape[0]
    pairs = [(srows_hbm.at[:, pl.ds(g * LANES, LANES)], srows.at[g]) for g in range(groups)]
    pairs += [(scnt_hbm, scnt), (lidx_hbm, lidx), (lcnt_hbm, lcnt), (hidx_hbm, hidx), (hcnt_hbm, hcnt)]
    tables = [
        pltpu.make_async_copy(src, dst, index_sem.at[i]) for i, (src, dst) in enumerate(pairs)
    ]
    first_tables, other_tables = tables[: groups + 1], tables[groups + 1 :]

    def w_load():
        mine = pl.ds(pl.multiple_of(d * shard, shard), shard)
        return pltpu.make_async_copy(weight_hbm.at[mine], wfull.at[z, d], wl_sem)

    for copy in first_tables:
        copy.start()
    for i in range(pieces):
        feat_copy(i).start()
    w_load().start()
    for copy in other_tables:
        copy.start()
    lv_copy = pltpu.make_async_copy(lvals_hbm, lvals, vals_sem.at[0])
    hv_copy = pltpu.make_async_copy(hvals_hbm, hvals, vals_sem.at[1])

    barrier = pltpu.get_barrier_semaphore()
    for o in range(1, n_dom):
        pl.semaphore_signal(barrier, inc=1, device_id=(lax.rem(d + o, n_dom), z), device_id_type=MESH)
    for o in range(1, n_col):
        pl.semaphore_signal(barrier, inc=1, device_id=(d, lax.rem(z + o, n_col)), device_id_type=MESH)
    bfull[z] = jnp.broadcast_to(bias_ref[...].reshape(1, width), bfull.shape[1:])

    def slots_of(k, q):
        count = outs[k].shape[1]
        return pl.ds(q * count, count)

    for k in range(3):
        mine = slots_of(k, d)
        lands[k][mine] = jnp.zeros((outs[k].shape[1], TILE, lanes), halo_late.dtype)
    acc[...] = jnp.zeros_like(acc)

    def widen(c, t):
        xf[c, pl.ds(pl.multiple_of(t * TILE, TILE), TILE), :] = xb[c][t].astype(jnp.float32)

    @pl.loop(0, pieces)
    def _(i):
        feat_copy(i).wait()
        for j in range(piece):
            widen(0, i * piece + j)

    lv_copy.start()
    hv_copy.start()
    late_copy().start()

    def widen_late():
        late_copy().wait()

        @pl.loop(0, pieces)
        def _(i):
            for j in range(piece):
                widen(1, i * piece + j)

    def peer_of(i):
        later = i // n_chips
        at_mate = (i + 1) // n_chips - later
        over = 2 * lax.rem(chip + lax.rem(i, n_chips) + 1, n_chips) + 1 - later
        return over - at_mate * core

    def halo_send(k, peer):
        return remote(
            outs[k].at[peer], lands[k].at[slots_of(k, d)], halo_s.at[k], halo_r.at[k], (peer, z)
        )

    def halo_all(k):
        most = outs[k].at[pl.ds(0, n_dom - 1)]
        return remote(most, most, halo_s.at[k], halo_r.at[k], (mate, z))

    def first_lanes(shape):
        return lax.broadcasted_iota(jnp.int32, shape, len(shape) - 1) < lanes // 2

    def swap(x):
        return pltpu.roll(x, lanes // 2, x.ndim - 1)

    def fold(low, high):
        first, turned = first_lanes(low.shape), swap(high)
        return jnp.where(first, low, turned), jnp.where(first, turned, low)

    def unfold(a, b):
        first = first_lanes(a.shape)
        return jnp.where(first, a, b), swap(jnp.where(first, b, a))

    def picked_rows(c, peer):
        @pl.loop(0, slot_total // LANES)
        def _(g):
            group = pl.ds(pl.multiple_of(g * LANES, LANES), LANES)
            into = stage.at[group]
            for k in range(LANES):
                into[k] = xf[c, srows[g, peer, k]]

        used = lax.broadcasted_iota(jnp.int32, (slot_total, lanes), 0) < scnt[0, peer]
        return jnp.where(used, stage[...], 0.0)

    def gather_early(peer):
        sent = picked_rows(0, peer)
        a, b = fold(sent[: slot_total // 2], sent[slot_total // 2 :])
        out_a[peer] = a.astype(out_a.dtype).reshape(half_peer, TILE, lanes)
        out_b[peer] = b.astype(out_b.dtype).reshape(half_peer, TILE, lanes)

    def gather_late():
        @pl.loop(0, n_dom - 1)
        def _(i):
            peer = peer_of(i)
            sent = picked_rows(1, peer)
            out_late[peer] = sent.astype(out_late.dtype).reshape(per_peer, TILE, lanes)
            halo_send(2, peer).start()

    def w_copy(o):
        return remote(wfull.at[z, d], wfull.at[z, d], w_s, w_r, (d, lax.rem(z + o, n_col)))

    def w_copies():
        some = pl.ds(0, n_col - 1)
        return remote(wfull.at[some, d], wfull.at[some, d], w_s, w_r, (d, lax.rem(z + 1, n_col)))

    def w_pass(o):
        return remote(wfull.at[:, d], wfull.at[:, d], wp_s, wp_r, (lax.rem(d + o, n_dom), z))

    def w_passes():
        most = pl.ds(0, n_dom - 1)
        return remote(wfull.at[:, most], wfull.at[:, most], wp_s, wp_r, (mate, z))

    def b_copy(o):
        return remote(bfull.at[z], bfull.at[z], b_s, b_r, (d, lax.rem(z + o, n_col)))

    def b_copies():
        some = bfull.at[pl.ds(0, n_col - 1)]
        return remote(some, some, b_s, b_r, (d, lax.rem(z + 1, n_col)))

    for copy in first_tables:
        copy.wait()
    gather_early(peer_of(0))
    pl.semaphore_wait(barrier, n_dom - 1 + n_col - 1)
    halo_send(0, peer_of(0)).start()
    w_load().wait()
    for o in range(1, n_col):
        w_copy(o).start()
        b_copy(o).start()

    @pl.loop(1, n_chips - 1)
    def _(i):
        gather_early(peer_of(i))
        halo_send(0, peer_of(i)).start()

    @pl.loop(0, n_chips - 1)
    def _(i):
        halo_send(1, peer_of(i)).start()


    @pl.loop(n_chips - 1, n_dom - 1)
    def _(i):
        gather_early(peer_of(i))
        halo_send(0, peer_of(i)).start()
        halo_send(1, peer_of(i)).start()

    @pl.when(core == 0)
    def _():
        widen_late()
        gather_late()

    for copy in other_tables:
        copy.wait()
    lv_copy.wait()
    hv_copy.wait()

    def kept(count, k):
        one = jnp.minimum(jnp.maximum(count - k, 0), 1).astype(jnp.float32)
        return jnp.broadcast_to(one, (TILE, TILE)).astype(jnp.bfloat16)

    def tile_rows(c, t):
        lhs, rhs = [], []
        n_loc, n_hal = lcnt[0, t], hcnt[0, t]
        for k in range(k_local):
            lhs.append(lvals[t, k] * kept(n_loc, k))
            rhs.append(xb[c][lidx[k, t]])
        for k in range(k_halo):
            lhs.append(hvals[t, k] * kept(n_hal, k))
            rhs.append(halos[c][hidx[k, t]])
        return jnp.dot(
            jnp.concatenate(lhs, axis=1),
            jnp.concatenate(rhs, axis=0),
            preferred_element_type=jnp.float32,
        )

    def p1_copy(c, s, o):
        return remote(
            tx.at[s, o - 1, c], rx.at[s, z, c], p1_s, p1_r.at[s], (d, lax.rem(z + o, n_col))
        )

    def p1_step(s):
        whole = tx.at[s]
        return remote(whole, whole, p1_s, p1_r.at[s], (d, lax.rem(z + 1, n_col)))

    def p1_part(s, o, k):
        at = pl.ds(k * (r_chunk // 2), r_chunk // 2)
        return remote(
            tx.at[s, o - 1, 0, at],
            rx.at[s, z, 0, at],
            p1_s,
            p1_r.at[s],
            (d, lax.rem(z + o, n_col)),
        )

    def folded(s, q, k):
        tiles = [tile_rows(0, q * tiles_q + s * ct + i) for i in range(ct)]
        pairs = [fold(tiles[i], tiles[i + ct // 2])[k] for i in range(ct // 2)]
        return jnp.concatenate(pairs, axis=0).astype(jnp.bfloat16)

    def early_step(s, k):
        at = pl.ds(k * (r_chunk // 2), r_chunk // 2)
        for o in range(1, n_col):
            tx[s, o - 1, 0, at, :] = folded(s, lax.rem(z + o, n_col), k)
            p1_part(s, o, k).start()

    def own_step(s):
        for k in range(2):
            at = pl.ds(k * (r_chunk // 2), r_chunk // 2)
            rx[s, z, 0, at, :] = folded(s, z, k)

    def full_step(c, s):
        for o in range(1, n_col):
            q = lax.rem(z + o, n_col)
            for i in range(ct):
                rows_i = tile_rows(c, q * tiles_q + s * ct + i)
                tx[s, o - 1, c, i * TILE : (i + 1) * TILE, :] = rows_i.astype(jnp.bfloat16)
            p1_copy(c, s, o).start()
        for i in range(ct):
            rows_i = tile_rows(c, z * tiles_q + s * ct + i)
            rx[s, z, c, i * TILE : (i + 1) * TILE, :] = rows_i.astype(jnp.bfloat16)

    def halves_of(land, q):
        return land[slots_of(0, q)].astype(jnp.float32)

    def place(q, k, tiles):
        at = pl.ds(q * per_peer + k * half_peer, half_peer)
        halo_early[at] = tiles.astype(halo_early.dtype)

    halo_all(0).wait_recv()

    @pl.loop(0, n_dom)
    def _(q):
        a = halves_of(land_a, q)
        place(q, 0, a)
        place(q, 1, swap(a))

    @pl.loop(0, EARLY_STEPS)
    def _(s):
        early_step(s, 0)

    halo_all(1).wait_recv()

    @pl.loop(0, n_dom)
    def _(q):
        low, high = unfold(halves_of(land_a, q), halves_of(land_b, q))
        place(q, 0, low)
        place(q, 1, high)

    @pl.loop(0, EARLY_STEPS)
    def _(s):
        early_step(s, 1)

    @pl.loop(EARLY_STEPS, steps)
    def _(s):
        full_step(0, s)

    @pl.loop(0, EARLY_STEPS)
    def _(s):
        own_step(s)

    @pl.when(core == 1)
    def _():
        widen_late()
        gather_late()

    w_copies().wait_recv()

    @pl.loop(1, n_dom)
    def _(o):
        w_pass(o).start()

    halo_all(2).wait_recv()

    @pl.loop(0, steps)
    def _(s):
        full_step(1, s)

    w_passes().wait_recv()
    b_copies().wait()

    def out_rows(s):
        return pl.ds(pl.multiple_of(z * rows_q + s * r_out, r_out), r_out)

    def p2_copy(s, o):
        q = lax.rem(z + o, n_col)
        return remote(tx2.at[s, q], out_hbm.at[out_rows(s)], p2_s, p2_r, (d, q))

    def p2_all():
        most = tx2.at[:, pl.ds(0, n_col - 1)]
        return remote(most, most, p2_s, p2_r, (d, lax.rem(z + 1, n_col)))

    def own_copy(s):
        return pltpu.make_async_copy(tx2.at[s, z], out_hbm.at[out_rows(s)], own_sem)

    def own_all():
        mine = tx2.at[:, z]
        return pltpu.make_async_copy(mine, mine, own_sem)

    @pl.loop(0, steps)
    def _(s):
        p1_step(s).wait_recv()

        @pl.when(s < EARLY_STEPS)
        def _():
            for j in range(n_col):
                a = rx[s, j, 0, : r_chunk // 2, :].astype(jnp.float32)
                b = rx[s, j, 0, r_chunk // 2 :, :].astype(jnp.float32)
                low, high = unfold(a, b)
                rx[s, j, 0, : r_chunk // 2, :] = low.astype(jnp.bfloat16)
                rx[s, j, 0, r_chunk // 2 :, :] = high.astype(jnp.bfloat16)

        @pl.loop(0, halves)
        def _(h):
            k = s * halves + h
            at = pl.ds(pl.multiple_of(h * r_out, r_out), r_out)
            mixed = jnp.concatenate(
                [rx[s, j, c, at, :] for j in range(n_col) for c in range(n_part)], axis=1
            )
            power = jnp.zeros((r_out, 1), jnp.float32)
            active = []
            for j in range(n_col):
                y = jnp.dot(
                    mixed, wfull[j].reshape(f_total, width), preferred_element_type=jnp.float32
                )
                y = jnp.maximum(y + bfull[j][0:1, :].astype(jnp.float32), 0.0)
                power = power + jnp.sum(y * y, axis=1, keepdims=True)
                active.append(y)
            factor = lax.rsqrt(power / f_total + epsilon)
            for j in range(n_col):
                scaled = active[j] * factor
                tx2[k, j] = scaled.astype(jnp.bfloat16)
                grouped = scaled.reshape(r_out // 8, 8, width)
                acc[j, 0] += jnp.sum(grouped, axis=0)
                acc[j, 1] += jnp.sum(grouped * grouped, axis=0)
            for o in range(1, n_col):
                p2_copy(k, o).start()
            own_copy(k).start()

    for j in range(n_col):
        part[j] = jnp.concatenate(
            [
                jnp.sum(acc[j, 0], axis=0, keepdims=True),
                jnp.sum(acc[j, 1], axis=0, keepdims=True),
                jnp.zeros((6, width), jnp.float32),
            ],
            axis=0,
        )

    def sd_copy(o):
        return remote(part, part_in.at[o], sd_s, sd_r, (lax.rem(d + o, n_dom), z))

    def sd_all():
        most = part_in.at[pl.ds(1, n_dom - 1)]
        return remote(most, most, sd_s, sd_r, (mate, z))

    @pl.loop(1, n_dom)
    def _(o):
        sd_copy(o).start()

    part_in[0] = part[...]
    sd_all().wait()
    colpart[...] = jnp.sum(part_in[...], axis=0)

    def sc_copy(o):
        q = lax.rem(z + o, n_col)
        return remote(colpart.at[q], colpart_in.at[o], sc_s, sc_r, (d, q))

    def sc_all():
        some = colpart_in.at[pl.ds(1, n_col - 1)]
        return remote(some, some, sc_s, sc_r, (d, lax.rem(z + 1, n_col)))

    for o in range(1, n_col):
        sc_copy(o).start()
    colpart_in[0] = colpart[z]

    w_copies().wait_send()
    w_passes().wait_send()
    for k in range(3):
        halo_all(k).wait_send()

    remote(tx, tx, p1_s, p1_r.at[0], (d, lax.rem(z + 1, n_col))).wait_send()
    sc_all().wait()
    totals = jnp.sum(colpart_in[...], axis=0) / node_total
    mean = totals[0:1, :]
    stat_ref[...] = jnp.concatenate([mean, totals[1:2, :] - mean * mean], axis=0)

    p2_all().wait()
    own_all().wait()


def flush(rows_ref, stat_ref, out_hbm, stat_hbm, row_sem, stat_sem):
    small = pltpu.make_async_copy(stat_ref, stat_hbm, stat_sem)
    small.start()
    piece = out_hbm.shape[0] // 8
    for i in range(8):
        at = pl.ds(i * piece, piece)
        pltpu.make_async_copy(rows_ref.at[at], out_hbm.at[at], row_sem).start()
    pltpu.make_async_copy(rows_ref, out_hbm, row_sem).wait()
    small.wait()


def on_device(
    features,
    weight,
    out_bias,
    local_index,
    local_count,
    local_vals,
    halo_index,
    halo_count,
    halo_vals,
    send_rows,
    send_count,
):
    rows, width = features.shape
    n_dom = lax.axis_size("dom")
    n_col = lax.axis_size("col")
    slot_total = send_rows.shape[2]
    f_total = weight.shape[0]
    n_part = width // LANES
    steps = rows // TILE // n_col // P1_TILES
    steps_out = rows // TILE // n_col // P2_TILES
    r_chunk = P1_TILES * TILE
    r_out = P2_TILES * TILE
    pieces = 8 if rows // TILE % 8 == 0 else 1
    any_spec = pl.BlockSpec(memory_space=pl.ANY)
    vmem = pl.BlockSpec(memory_space=pltpu.VMEM)
    bf16, f32 = jnp.bfloat16, jnp.float32
    dma = pltpu.SemaphoreType.DMA

    def table(*shape):
        return pltpu.SMEM(shape, jnp.int32)

    halo_bytes = 4 * n_dom * slot_total * width
    grant = 44 * 2**20 + 2 * halo_bytes
    held = pltpu.VMEM if grant + 2 * rows * width < 58 * 2**20 else jax.ShapeDtypeStruct
    grant = grant if held is pltpu.VMEM else 67043328
    normalized, stats = pl.pallas_call(
        functools.partial(kernel, n_dom, n_col, rows * n_dom),
        out_shape=(
            held((rows, width), bf16),
            held((2, width), f32),
        ),
        in_specs=[any_spec, any_spec, vmem] + [any_spec] * 8,
        out_specs=(any_spec, vmem),
        scratch_shapes=[
            pltpu.VMEM((rows // TILE, TILE, LANES), bf16),
            pltpu.VMEM((rows // TILE, TILE, LANES), bf16),
            pltpu.VMEM((n_part, rows, LANES), f32),
            pltpu.VMEM((slot_total, LANES), f32),
            pltpu.VMEM((n_dom, slot_total // TILE // 2, TILE, LANES), bf16),
            pltpu.VMEM((n_dom, slot_total // TILE // 2, TILE, LANES), bf16),
            pltpu.VMEM((n_dom, slot_total // TILE, TILE, LANES), bf16),
            pltpu.VMEM((n_dom * slot_total // TILE // 2, TILE, LANES), bf16),
            pltpu.VMEM((n_dom * slot_total // TILE // 2, TILE, LANES), bf16),
            pltpu.VMEM((n_dom * slot_total // TILE, TILE, LANES), bf16),
            pltpu.VMEM((n_dom * slot_total // TILE, TILE, LANES), bf16),
            pltpu.VMEM(local_vals.shape[1:], bf16),
            pltpu.VMEM(halo_vals.shape[1:], bf16),
            pltpu.VMEM((n_col, n_dom, f_total // n_dom, width), bf16),
            pltpu.VMEM((n_col, 16, width), bf16),
            pltpu.VMEM((steps, n_col - 1, n_part, r_chunk, LANES), bf16),
            pltpu.VMEM((steps, n_col, n_part, r_chunk, LANES), bf16),
            pltpu.VMEM((steps_out, n_col, r_out, width), bf16),
            pltpu.VMEM((n_col, 2, 8, width), f32),
            pltpu.VMEM((n_col, 8, width), f32),
            pltpu.VMEM((n_dom, n_col, 8, width), f32),
            pltpu.VMEM((n_col, 8, width), f32),
            pltpu.VMEM((n_col, 8, width), f32),
            table(local_index.shape[2], rows // TILE),
            table(1, rows // TILE),
            table(halo_index.shape[2], rows // TILE),
            table(1, rows // TILE),
            table(slot_total // LANES, n_dom, LANES),
            table(1, n_dom),
            dma((pieces,)),
            dma,
            dma((slot_total // LANES + 5,)),
            dma((2,)),
            dma,
            dma((3,)),
            dma((3,)),
            dma,
            dma,
            dma,
            dma,
            dma,
            dma,
            dma,
            dma((steps,)),
            dma,
            dma,
            dma,
            dma,
            dma,
            dma,
            dma,
        ],
        compiler_params=pltpu.CompilerParams(
            collective_id=0, has_side_effects=True, vmem_limit_bytes=grant
        ),
    )(
        features.reshape(rows // TILE, TILE, width),
        weight,
        out_bias,
        local_index[0].T,
        local_count,
        local_vals[0],
        halo_index[0].T,
        halo_count,
        halo_vals[0],
        send_rows[0],
        send_count,
    )
    if held is not pltpu.VMEM:
        return normalized, stats
    return pl.pallas_call(
        flush,
        out_shape=(
            jax.ShapeDtypeStruct((rows, width), bf16),
            jax.ShapeDtypeStruct((2, width), f32),
        ),
        in_specs=[vmem, vmem],
        out_specs=(any_spec, any_spec),
        scratch_shapes=[dma, dma],
        compiler_params=pltpu.CompilerParams(vmem_limit_bytes=16 * 2**20),
    )(normalized, stats)


def solution(mesh):
    in_specs = (
        P("dom", "col"),
        P(None, "col"),
        P("col"),
        P("dom", None, None),
        P("dom", None),
        P("dom", None, None, None, None),
        P("dom", None, None),
        P("dom", None),
        P("dom", None, None, None, None),
        P("dom", None, None),
        P("dom", None),
    )
    out_specs = (P("dom", "col"), P(None, "col"))
    return jax.shard_map(
        on_device, mesh=mesh, in_specs=in_specs, out_specs=out_specs, check_vma=False
    )
```
